128 devices in a mesh: dp: 8 (over x, core), feat: 16 (over y, z).
Axes of the slice: x: 4, y: 4, z: 4, core: 2. Of those that a mesh axis runs over, the one named last changes fastest.
Arguments:
- features: bfloat16 [262144, 2048], P('dp', 'feat'), may hold values from -210 to 210
- labels: int32 [262144], P('dp'), may hold values from 0 to 63
- groups: int32 [262144], P('dp'), may hold values from 0 to 1023
- coefficients: float32 [2048, 64], P('feat'), may hold values from -0.125 to 0.125
- coef_momentum: float32 [2048, 64], P('feat'), may hold values from -6 to 6
- group_effects: float32 [1024, 64], P('feat'), may hold values from -4 to 4
- group_momentum: float32 [1024, 64], P('feat'), may hold values from -6 to 6
- log_scale: float32 [64], replicated, may hold values from -1.2 to 0.4
Outputs:
- new_coefficients: float32 [2048, 64], P('feat')
- new_coef_momentum: float32 [2048, 64], P('feat')
- new_group_effects: float32 [1024, 64], P('feat')
- new_group_momentum: float32 [1024, 64], P('feat')
- energy_change: float32 [], replicated
The draws below stay inside these ranges and needn't reach their ends.
All inputs are finite; a program needn't handle non-finite values.
Results may differ from the reference program's by a relative error of at most 0.001.
The reference program's roundings to bfloat16 on the way (of `residual`) count: a program that leaves them out, or rounds other values in their place, can miss the bound.
Values may be sent and summed in bfloat16 or wider, within the bound.
A program may use at most 128 MiB of HBM per device.

```python
import math
import jax
import jax.numpy as jnp
import numpy as np
from jax import lax

F = 2048
K = 64
G = 1024
ROW_DEV = 32768
ROWS = 262144
N_FEAT = 16


def draw_features(key, part):
    first_key, second_key, third_key = jax.random.split(key, 3)
    values = jax.random.normal(first_key, (ROWS, F), jnp.float32)
    return jnp.clip(values, -6.0, 6.0).astype(jnp.bfloat16)


def plant(values, own_key, low, high):
    index_at = [jax.random.randint(jax.random.fold_in(own_key, axis), (), 0, length) for axis, length in enumerate(values.shape)]
    main_axis = values.shape.index(max(values.shape))
    neighbour = index_at[:main_axis] + [(index_at[main_axis] + 1) % values.shape[main_axis]] + index_at[main_axis + 1:]
    return values.at[tuple(index_at)].set(low).at[tuple(neighbour)].set(high)


def steps_of(own_key, dims, pieces, low, high):
    factor_of, own = 1.0, jax.random.fold_in(own_key, 6)
    for position, parts in pieces:
        steps = jnp.exp(jax.random.uniform(jax.random.fold_in(own, position), (parts,), jnp.float32, low / len(pieces), high / len(pieces)))
        factor_of = factor_of * jnp.repeat(steps, dims[position] // parts).reshape([-1 if axis == position else 1 for axis in range(len(dims))])
    return factor_of


def rank_table(count, slope):
    portions = [(1 << 20) // math.isqrt(grade ** slope) + 1 for grade in range(1, count + 1)]
    deviation = 1 + sum(portions) // (1 << 30)
    return np.cumsum(np.array([max(1, weight // deviation) for weight in portions]))


def ranked(stream_key, dims, amount, lean):
    grid = rank_table(amount, lean)
    lot = jax.random.randint(jax.random.fold_in(stream_key, 1), dims, 0, int(grid[amount - 1]))
    rank = jnp.searchsorted(jnp.asarray(grid, jnp.int32), lot, side="right")
    return jax.random.permutation(jax.random.fold_in(stream_key, 2), amount)[rank].astype(jnp.int32)


def normal_values(own_key, extent, spread, limit, cuts=(), kind=jnp.bfloat16):
    loudness = steps_of(own_key, extent, cuts, -0.22, 0.18) if cuts else 1.0
    entries = jax.random.normal(own_key, extent, jnp.float32) * spread * loudness
    return jnp.minimum(jnp.maximum(entries, -limit), limit).astype(kind)


def setup_inputs(seed: int = 0) -> dict:
    seeds = jax.random.split(jax.random.key(seed), 9)
    return {
        "features": draw_features(jax.random.fold_in(seeds[8], 71), 0),
        "labels": plant(jax.random.randint(seeds[1], (ROWS,), 0, K), jax.random.fold_in(seeds[1], 1), 0, K - 1).astype(jnp.int32),
        "groups": plant(ranked(seeds[2], (ROWS,), G, 1), jax.random.fold_in(seeds[2], 3), 0, G - 1).astype(jnp.int32),
        "coefficients": normal_values(seeds[3], (F, K), F ** -0.5, 0.125, ((0, 16),), jnp.float32),
        "coef_momentum": normal_values(seeds[4], (F, K), 1.0, 6.0, ((0, 16),), jnp.float32),
        "group_effects": normal_values(seeds[5], (G, K), 0.5, 4.0, ((0, 16),), jnp.float32),
        "group_momentum": normal_values(seeds[6], (G, K), 1.0, 6.0, ((0, 16),), jnp.float32),
        "log_scale": jnp.clip(jax.random.uniform(seeds[7], (K,), jnp.float32, -1.2, 0.4), -1.2, 0.4),
    }


def row_terms(logits, labels):
    largest = lax.optimization_barrier(jnp.max(logits, axis=1, keepdims=True))
    shifted = logits - largest
    scaled = jnp.exp(shifted)
    normalizer = lax.optimization_barrier(jnp.sum(scaled, axis=1, keepdims=True))
    probability = scaled / normalizer
    target = (labels[:, None] == jnp.arange(K, dtype=jnp.int32)[None, :]).astype(jnp.float32)
    loglik = lax.optimization_barrier(jnp.sum(target * shifted, axis=1)) - jnp.log(normalizer[:, 0])
    residual = (target - probability).astype(jnp.bfloat16).astype(jnp.float32)
    return (loglik, residual)

def evaluate(features, labels, groups, coefficients, group_effects):
    block_rows = ROW_DEV // N_FEAT
    block_count = ROWS // block_rows
    feat_block = F // N_FEAT
    group_block = G // N_FEAT
    coef_low = coefficients.astype(jnp.bfloat16).astype(jnp.float32).reshape(N_FEAT, feat_block, K)
    group_low = group_effects.astype(jnp.bfloat16).astype(jnp.float32).reshape(N_FEAT, group_block, K)
    highest = lax.Precision.HIGHEST

    def advance(totals, block_index):
        offset = (block_index * block_rows).astype(jnp.int32)
        rows_x = lax.dynamic_slice_in_dim(features, offset, block_rows, 0).astype(jnp.float32)
        rows_l = lax.dynamic_slice_in_dim(labels, offset, block_rows, 0)
        rows_g = lax.dynamic_slice_in_dim(groups, offset, block_rows, 0)
        onehot = (rows_g[:, None] == jnp.arange(G, dtype=jnp.int32)[None, :]).astype(jnp.float32)
        partial_value = jnp.einsum('nfi,fik->fnk', rows_x.reshape(block_rows, N_FEAT, feat_block), coef_low, precision=highest)
        partial_value = partial_value + jnp.einsum('nfg,fgk->fnk', onehot.reshape(block_rows, N_FEAT, group_block), group_low, precision=highest)
        logits = lax.optimization_barrier(jnp.sum(partial_value, axis=0))
        loglik, residual = row_terms(logits, rows_l)
        coef_grad = totals[0] + jnp.einsum('ni,nk->ik', rows_x, residual, precision=highest)
        group_grad = totals[1] + jnp.einsum('ng,nk->gk', onehot, residual, precision=highest)
        return ((coef_grad, group_grad), loglik)
    initial = (jnp.zeros((F, K), jnp.float32), jnp.zeros((G, K), jnp.float32))
    (coef_grad, group_grad), loglik = lax.scan(advance, initial, jnp.arange(block_count, dtype=jnp.int32))
    return (loglik, coef_grad, group_grad)

def reference(features, labels, groups, coefficients, coef_momentum, group_effects, group_momentum, log_scale):
    step_coef = 4.0 / math.sqrt(ROWS)
    step_group = 4.0 * math.sqrt(G / ROWS)
    inv_var = jnp.exp(-2.0 * log_scale)
    loglik_old, coef_grad, group_grad = evaluate(features, labels, groups, coefficients, group_effects)
    coef_half = coef_momentum + 0.5 * step_coef * (coef_grad - coefficients)
    group_half = group_momentum + 0.5 * step_group * (group_grad - group_effects * inv_var)
    coef_new = coefficients + step_coef * coef_half
    group_new = group_effects + step_group * group_half
    loglik_new, coef_grad, group_grad = evaluate(features, labels, groups, coef_new, group_new)
    coef_mom_new = coef_half + 0.5 * step_coef * (coef_grad - coef_new)
    group_mom_new = group_half + 0.5 * step_group * (group_grad - group_new * inv_var)
    energy = jnp.sum(loglik_old - loglik_new)
    energy = energy + 0.5 * jnp.sum(coef_new * coef_new - coefficients * coefficients)
    energy = energy + 0.5 * jnp.sum((group_new * group_new - group_effects * group_effects) * inv_var)
    energy = energy + 0.5 * jnp.sum(coef_mom_new * coef_mom_new - coef_momentum * coef_momentum)
    energy = energy + 0.5 * jnp.sum(group_mom_new * group_mom_new - group_momentum * group_momentum)
    return (coef_new, coef_mom_new, group_new, group_mom_new, energy)
```

```python
import math

import jax
import jax.numpy as jnp
from jax import lax
from jax.experimental import pallas as pl
from jax.experimental.pallas import tpu as pltpu
from jax.sharding import Mesh
from jax.sharding import PartitionSpec as P

FEAT = ("feat_0", "feat_1")
DP = ("dp_0", "dp_1")

NC = 4
UNIT = 128
BF16, F32 = jnp.bfloat16, jnp.float32
NT = (((1,), (1,)), ((), ()))
NN = (((1,), (0,)), ((), ()))


def dot(a, b, dims):
    return lax.dot_general(a, b, dims, preferred_element_type=F32)


def kernel(rows_total, group_total, feats, labels, groups, pos_ref, mom_ref, iv_ref,
           new_ref, mom_out_ref, energy_ref,
           X, ST, OH, W, PL, R1, R2, RG, CS, CG, ACC, GS, GR, DS, DR, DG, EN, LL, HALF,
           loc_sem, a_s, a_r, rs_s, rs_r, g_s, g_r, c_s, c_r, q_s, q_r, d_s, d_r, b_s, b_r, e_s, e_r):
    x, core = lax.axis_index("dp_0"), lax.axis_index("dp_1")
    place = (lax.axis_index("feat_0"), lax.axis_index("feat_1"))
    dp = x * 2 + core
    classes = pos_ref.shape[0] - 32
    block_rows = NC * 8 * UNIT
    chunk_rows = 8 * UNIT

    def at(axis, step):
        return {FEAT[axis]: lax.rem(place[axis] + step, 4)}

    def dp_at(step):
        peer = lax.rem(dp + step, 8)
        return {"dp_0": peer // 2, "dp_1": lax.rem(peer, 2)}

    def remote(src, dst, s, r, device):
        return pltpu.make_async_remote_copy(
            src_ref=src, dst_ref=dst, send_sem=s, recv_sem=r,
            device_id=device, device_id_type=pl.DeviceIdType.MESH)

    def a2a(t, c, k):
        me = place[t]
        half = chunk_rows // 2

        def rows(step, part, count):
            first = (t * 4 + lax.rem(me + step, 4)) * block_rows + c * chunk_rows + part * half
            return feats.at[pl.ds(pl.multiple_of(first, half), count)]

        def to(r, part, count):
            return X.at[t, r, pl.ds(pl.multiple_of(c * chunk_rows + part * half, half), count)]

        sems = (a_s.at[t, c, k], a_r.at[t, c, k])
        if k == 0:
            return remote(rows(1, 0, chunk_rows), to(3, 0, chunk_rows), *sems, at(t, 1))
        if k == 1:
            return remote(rows(3, 0, chunk_rows), to(1, 0, chunk_rows), *sems, at(t, 3))
        if k == 2:
            return remote(rows(2, 0, half), ST.at[t, c, 0], *sems, at(t, 1))
        if k == 3:
            return remote(rows(2, 1, half), ST.at[t, c, 1], *sems, at(t, 3))
        if k == 4:
            return remote(ST.at[t, c, 0], to(2, 0, half), *sems, at(t, 1))
        return remote(ST.at[t, c, 1], to(2, 1, half), *sems, at(t, 3))

    def scatter(e, t, c, k):
        axis = 1 - t
        p = place[axis]
        step = 1 if k % 2 == 0 else 3
        owner = lax.rem(p + (2 if k < 2 else step), 4)
        h = (0, 1, 1, 0, 0, 1)[k]
        dst = R1.at[e, t, c, k] if k < 2 else R2.at[e, t, c, k % 2, h]
        return remote(PL.at[e, t, c, owner * 2 + h], dst, rs_s.at[e, t, c, k], rs_r.at[e, t, c, k], at(axis, step))

    def gather(e, t, c, k):
        axis = 1 - t
        p = place[axis]
        step = 1 if k % 2 == 0 else 3
        if k < 2:
            ref = RG.at[e, t, c, pl.ds(p * 2, 2)]
        else:
            ref = RG.at[e, t, c, lax.rem(p + 4 - step, 4) * 2 + (k - 2)]
        return remote(ref, ref, g_s.at[e, t, c, k], g_r.at[e, t, c, k], at(axis, step))

    def weights(e, t, r):
        return remote(CS.at[e], CG.at[e, t, 3 - r], c_s.at[e, t, r - 1], c_r.at[e, t, r - 1], at(t, r))

    def gradients(e, t, r):
        return remote(GS.at[e, t, r], GR.at[e, t, r - 1], q_s.at[e, t, r - 1], q_r.at[e, t, r - 1], at(t, r))

    def dp_scatter(e, k):
        return remote(DS.at[e, lax.rem(dp + k, 8)], DR.at[e, k - 1], d_s.at[e, k - 1], d_r.at[e, k - 1], dp_at(k))

    def dp_gather(e, k):
        return remote(DG.at[e, dp], DG.at[e, dp], b_s.at[e, k - 1], b_r.at[e, k - 1], dp_at(k))

    def energies(k):
        mine = place[0] * 4 + place[1]
        device = {**at(0, k // 4), **at(1, k % 4)}
        return remote(EN.at[mine], EN.at[mine], e_s.at[k - 1], e_r.at[k - 1], device)

    barrier = pltpu.get_barrier_semaphore()
    for k in range(1, 16):
        pl.semaphore_signal(barrier, inc=1, device_id={**at(0, k // 4), **at(1, k % 4)},
                            device_id_type=pl.DeviceIdType.MESH)
    for k in range(1, 8):
        pl.semaphore_signal(barrier, inc=1, device_id=dp_at(k), device_id_type=pl.DeviceIdType.MESH)

    def own(t):
        first = (t * 4 + place[t]) * block_rows
        return pltpu.make_async_copy(feats.at[pl.ds(pl.multiple_of(first, block_rows), block_rows)], X.at[t, 0],
                                     loc_sem.at[t])

    own(0).start()
    own(1).start()
    CS[0] = pos_ref[...].astype(BF16)
    pl.semaphore_wait(barrier, 22)

    lane = lax.broadcasted_iota(jnp.int32, (32, 128), 1)
    low = lane < 64

    def send_weights(e):
        for t in range(2):
            for r in (1, 3, 2):
                weights(e, t, r).start()

    def gather_weights(e):
        for t in range(2):
            for r in (1, 3, 2):
                weights(e, t, r).wait_recv()
            packed = []
            for r in range(4):
                block = CS[e] if r == 0 else CG[e, t, r - 1]
                W[t, :, r * 128:(r + 1) * 128] = block[:classes]
                packed.append(block[classes:].astype(F32))
            for i in range(2):
                a, b = packed[2 * i], packed[2 * i + 1]
                lanes = pl.ds(512 + i * 128, 128)
                W[t, 0:32, lanes] = jnp.where(low, a, pltpu.roll(b, 64, 1)).astype(BF16)
                W[t, 32:64, lanes] = jnp.where(low, pltpu.roll(a, 64, 1), b).astype(BF16)

    def send_features(c):
        for k in (2, 3, 0, 1):
            for t in range(2):
                a2a(t, c, k).start()

    def pass_features(c):
        for k in (2, 3):
            for t in range(2):
                a2a(t, c, k).wait_recv()
                a2a(t, c, k + 2).start()

    def wait_features(c):
        for k in (0, 1, 4, 5):
            for t in range(2):
                a2a(t, c, k).wait_recv()

    def pair(t, r, rows):
        return jnp.concatenate([X[t, r, rows, :], X[t, r + 1, rows, :]], axis=1)

    def rows_of(c, o):
        return pl.ds(pl.multiple_of(c * chunk_rows + o * 256, 256), 256)

    def logits(e, c):
        for t in range(2):
            def block(o, _):
                rows = rows_of(c, o)
                total = dot(W[t, :, 0:256], pair(t, 0, rows), NT)
                total = total + dot(W[t, :, 256:512], pair(t, 2, rows), NT)
                total = total + dot(W[t, :, 512:768], OH[t, c * 4 + o], NN)
                PL[e, t, c, o * 2] = total[:, :128]
                PL[e, t, c, o * 2 + 1] = total[:, 128:]
                return 0
            lax.fori_loop(0, 4, block, 0)
            for k in range(4):
                scatter(e, t, c, k).start()

    def add_passed(e, c):
        for t in range(2):
            p = place[1 - t]
            for k in range(2):
                scatter(e, t, c, k).wait_recv()
                unit = lax.rem(p + (1 if k == 0 else 3), 4) * 2 + k
                PL[e, t, c, unit] = PL[e, t, c, unit] + R1[e, t, c, k]
            for k in (4, 5):
                scatter(e, t, c, k).start()

    def softmax(e, c):
        for t in range(2):
            p = place[1 - t]
            for k in range(2, 6):
                scatter(e, t, c, k).wait_recv()
            for h in range(2):
                value = PL[e, t, c, p * 2 + h] + R2[e, t, c, 0, h] + R2[e, t, c, 1, h]
                unit = ((t * 4 + place[t]) * NC + c) * 8 + p * 2 + h
                label = labels[pl.ds(unit, 1), :]
                shifted = value - jnp.max(value, axis=0, keepdims=True)
                scaled = jnp.exp(shifted)
                normalizer = jnp.sum(scaled, axis=0, keepdims=True)
                hit = lax.broadcasted_iota(jnp.int32, value.shape, 0) == label
                loglik = jnp.sum(jnp.where(hit, shifted, 0.0), axis=0, keepdims=True) - jnp.log(normalizer)
                LL[e, t, c, h] = jnp.broadcast_to(loglik, (8, 128))
                probability = scaled * (1.0 / normalizer)
                RG[e, t, c, p * 2 + h] = (jnp.where(hit, 1.0, 0.0) - probability).astype(BF16)
            for k in range(2):
                gather(e, t, c, k).start()

    def pass_residual(e, c):
        for t in range(2):
            for k in range(2):
                gather(e, t, c, k).wait_recv()
                gather(e, t, c, k + 2).start()

    def gradient(e, c):
        for t in range(2):
            for k in (2, 3):
                gather(e, t, c, k).wait_recv()

            def block(o, _):
                rows = rows_of(c, o)
                res = jnp.concatenate([RG[e, t, c, o * 2], RG[e, t, c, o * 2 + 1]], axis=1)
                ACC[t, :, 0:256] += dot(res, pair(t, 0, rows), NN)
                ACC[t, :, 256:512] += dot(res, pair(t, 2, rows), NN)
                ACC[t, :, 512:768] += dot(res, OH[t, c * 4 + o], NT)
                return 0
            lax.fori_loop(0, 4, block, 0)

    def reduce_gradient(e):
        for t in range(2):
            for r in (1, 3, 2, 0):
                GS[e, t, r, 0:classes] = ACC[t, :, r * 128:(r + 1) * 128]
                tile = 512 + (r // 2) * 128
                top, bottom = ACC[t, 0:32, tile:tile + 128], ACC[t, 32:64, tile:tile + 128]
                if r % 2 == 0:
                    GS[e, t, r, classes:] = jnp.where(low, top, pltpu.roll(bottom, 64, 1))
                else:
                    GS[e, t, r, classes:] = jnp.where(low, pltpu.roll(top, 64, 1), bottom)
                if r:
                    gradients(e, t, r).start()
        total = GS[e, 0, 0] + GS[e, 1, 0]
        for r in (1, 3, 2):
            for t in range(2):
                gradients(e, t, r).wait_recv()
                total = total + GR[e, t, r - 1]
        for i in range(6):
            DS[e, i] = total[i * 16:(i + 1) * 16]
        for k in range(1, 8):
            dp_scatter(e, k).start()
        mine = DS[e, dp]
        for k in range(1, 8):
            dp_scatter(e, k).wait_recv()
            mine = mine + DR[e, k - 1]
        DG[e, dp, 0:16] = mine
        for k in range(1, 8):
            dp_gather(e, k).start()
        for k in range(1, 8):
            dp_gather(e, k).wait_recv()
        return jnp.concatenate([DG[e, i, 0:16] for i in range(6)], axis=0)

    send_weights(0)
    send_features(0)

    for e in range(2):
        for i in (6, 7):
            DS[e, i] = jnp.zeros((16, 128), F32)
    DG[0, dp, 16:24] = jnp.zeros((8, 128), F32)

    ids = lax.broadcasted_iota(jnp.int32, (64, 128), 0)
    for t in range(2):
        def onehot(b, _):
            for h in range(2):
                unit = (t * 4 + place[t]) * (NC * 8) + b * 2 + h
                group = groups[pl.ds(unit, 1), :]
                for r in range(4):
                    other = lax.rem(place[t] + r, 4)
                    owner = other * 4 + place[1] if t == 0 else place[0] * 4 + other
                    hit = ids + owner * 64 == group
                    OH[t, b, r * 64:(r + 1) * 64, h * 128:(h + 1) * 128] = jnp.where(hit, 1.0, 0.0).astype(BF16)
            return 0
        lax.fori_loop(0, NC * 4, onehot, 0)
    gather_weights(0)
    ACC[...] = jnp.zeros_like(ACC)
    own(0).wait()
    own(1).wait()

    def slot(s, _):
        def stage(lag, body):
            c = s - lag
            pl.when(jnp.logical_and(c >= 0, c < NC))(lambda: body(c))
        stage(-1, send_features)
        stage(0, pass_features)

        def first(c):
            wait_features(c)
            logits(0, c)
        stage(1, first)
        stage(2, lambda c: add_passed(0, c))
        stage(3, lambda c: softmax(0, c))
        stage(4, lambda c: pass_residual(0, c))
        stage(5, lambda c: gradient(0, c))
        return 0
    lax.fori_loop(0, NC + 5, slot, 0)

    grad = reduce_gradient(0)
    row = lax.broadcasted_iota(jnp.int32, grad.shape, 0)
    step = jnp.where(row < classes, 4.0 / math.sqrt(rows_total), 4.0 * math.sqrt(group_total / rows_total))
    half = mom_ref[...] + 0.5 * step * (grad - pos_ref[...] * iv_ref[...])
    new = pos_ref[...] + step * half
    CS[1] = new.astype(BF16)
    send_weights(1)
    new_ref[...] = new
    HALF[...] = half

    ACC[...] = jnp.zeros_like(ACC)
    gather_weights(1)
    for body in (logits, add_passed, softmax, pass_residual, gradient):
        def over(c, _, body=body):
            body(1, c)
            return 0
        lax.fori_loop(0, NC, over, 0)

    change = jnp.zeros((8, 128), F32)
    for t in range(2):
        for c in range(NC):
            for h in range(2):
                change = change + (LL[0, t, c, h] - LL[1, t, c, h])
    DG[1, dp, 16:24] = change
    grad = reduce_gradient(1)
    half, new = HALF[...], new_ref[...]
    mom = half + 0.5 * step * (grad - new * iv_ref[...])
    mom_out_ref[...] = mom
    state = 0.5 * ((new * new - pos_ref[...] * pos_ref[...]) * iv_ref[...] + (mom * mom - mom_ref[...] * mom_ref[...]))
    terms = jnp.broadcast_to(jnp.sum(state, axis=0, keepdims=True), (8, 128))
    for i in range(8):
        terms = terms + DG[1, i, 16:24]
    EN[place[0] * 4 + place[1]] = terms
    for k in range(1, 16):
        energies(k).start()
    for k in range(1, 16):
        energies(k).wait_recv()
    terms = EN[0]
    for i in range(1, 16):
        terms = terms + EN[i]
    energy_ref[...] = jnp.broadcast_to(jnp.sum(terms, axis=1, keepdims=True), (8, 128))

    def sent(c, _):
        for t in range(2):
            for k in range(6):
                a2a(t, c, k).wait_send()
                for e in range(2):
                    scatter(e, t, c, k).wait_send()
                    if k < 4:
                        gather(e, t, c, k).wait_send()
        return 0
    lax.fori_loop(0, NC, sent, 0)
    for e in range(2):
        for t in range(2):
            for r in range(1, 4):
                weights(e, t, r).wait_send()
                gradients(e, t, r).wait_send()
        for k in range(1, 8):
            dp_scatter(e, k).wait_send()
            dp_gather(e, k).wait_send()
    for k in range(1, 16):
        energies(k).wait_send()


def packed(coef, group):
    turned = group.T
    return jnp.concatenate([coef.T, jnp.concatenate([turned[:32], turned[32:]], axis=1)], axis=0)


def unpacked(both, classes):
    tail = both[classes:]
    return both[:classes].T, jnp.concatenate([tail[:, :64], tail[:, 64:]], axis=0).T


def per_device(
    features, labels, groups, coefficients, coef_momentum, group_effects, group_momentum, log_scale
):
    rows = labels.shape[0]
    classes = coefficients.shape[1]
    rows_total = rows * lax.axis_size(DP)
    group_total = group_effects.shape[0] * lax.axis_size(FEAT)
    pos = packed(coefficients, group_effects)
    mom = packed(coef_momentum, group_momentum)
    inv_var = jnp.broadcast_to(jnp.exp(-2.0 * log_scale)[None, :], (64, classes))
    iv = packed(jnp.ones_like(coefficients), inv_var)
    vmem = pl.BlockSpec(memory_space=pltpu.VMEM)
    dma = pltpu.SemaphoreType.DMA
    new, new_mom, energy = pl.pallas_call(
        lambda *refs: kernel(rows_total, group_total, *refs),
        out_shape=[jax.ShapeDtypeStruct((96, 128), F32), jax.ShapeDtypeStruct((96, 128), F32),
                   jax.ShapeDtypeStruct((8, 128), F32)],
        in_specs=[pl.BlockSpec(memory_space=pl.ANY)] + [vmem] * 5,
        out_specs=[vmem] * 3,
        scratch_shapes=[
            pltpu.VMEM((2, 4, NC * 1024, 128), BF16),
            pltpu.VMEM((2, NC, 2, 512, 128), BF16),
            pltpu.VMEM((2, NC * 4, 256, 256), BF16),
            pltpu.VMEM((2, 64, 768), BF16),
            pltpu.VMEM((2, 2, NC, 8, 64, 128), F32),
            pltpu.VMEM((2, 2, NC, 2, 64, 128), F32),
            pltpu.VMEM((2, 2, NC, 2, 2, 64, 128), F32),
            pltpu.VMEM((2, 2, NC, 8, 64, 128), BF16),
            pltpu.VMEM((2, 96, 128), BF16),
            pltpu.VMEM((2, 2, 3, 96, 128), BF16),
            pltpu.VMEM((2, 64, 768), F32),
            pltpu.VMEM((2, 2, 4, 96, 128), F32),
            pltpu.VMEM((2, 2, 3, 96, 128), F32),
            pltpu.VMEM((2, 8, 16, 128), F32),
            pltpu.VMEM((2, 7, 16, 128), F32),
            pltpu.VMEM((2, 8, 24, 128), F32),
            pltpu.VMEM((16, 8, 128), F32),
            pltpu.VMEM((2, 2, NC, 2, 8, 128), F32),
            pltpu.VMEM((96, 128), F32),
            dma((2,)),
            dma((2, NC, 6)), dma((2, NC, 6)),
            dma((2, 2, NC, 6)), dma((2, 2, NC, 6)),
            dma((2, 2, NC, 4)), dma((2, 2, NC, 4)),
            dma((2, 2, 3)), dma((2, 2, 3)),
            dma((2, 2, 3)), dma((2, 2, 3)),
            dma((2, 7)), dma((2, 7)),
            dma((2, 7)), dma((2, 7)),
            dma((15,)), dma((15,)),
        ],
        compiler_params=pltpu.CompilerParams(
            collective_id=0, has_side_effects=True, vmem_limit_bytes=56 * 2**20),
        name="leapfrog",
    )(features, labels.reshape(-1, 128), groups.reshape(-1, 128), pos, mom, iv)
    new_coef, new_group = unpacked(new, classes)
    new_coef_mom, new_group_mom = unpacked(new_mom, classes)
    return (new_coef, new_coef_mom, new_group, new_group_mom, energy[0, 0])


def solution(mesh):
    torus = Mesh(mesh.devices.reshape(4, 2, 4, 4), ("dp_0", "dp_1", "feat_0", "feat_1"))
    in_specs = (
        P(DP, FEAT),
        P(DP),
        P(DP),
        P(FEAT, None),
        P(FEAT, None),
        P(FEAT, None),
        P(FEAT, None),
        P(),
    )
    out_specs = (P(FEAT, None), P(FEAT, None), P(FEAT, None), P(FEAT, None), P())
    return jax.shard_map(
        per_device, mesh=torus, in_specs=in_specs, out_specs=out_specs, check_vma=False
    )
```

```python
import math

import jax
import jax.numpy as jnp
from jax import lax
from jax.experimental import pallas as pl
from jax.experimental.pallas import tpu as pltpu
from jax.sharding import Mesh
from jax.sharding import PartitionSpec as P

FEAT = ("feat_0", "feat_1")
DP = ("dp_0", "dp_1")

NC = 4
LANES = 1024 // NC
CHUNK = 4 * LANES
BLOCK = NC * CHUNK
AHEAD = 1
BF16, F32 = jnp.bfloat16, jnp.float32


def dot(a, b):
    return lax.dot_general(a, b, (((1,), (0,)), ((), ())), preferred_element_type=F32)


def kernel(rows_total, group_total, feats, labels, groups, coef_ref, coef_mom_ref, group_ref, group_mom_ref,
           scale_ref, coef_out, coef_mom_out, group_out, group_mom_out, energy_ref,
           X, ST, XO, OHT, W, PL, R1, R2, RG, CS, CG, ACC, GS, GR, DA, DAR, DB, DC, EN, LL, DIFF,
           POS, MOM, IV, HALF, NEW, WIDE,
           loc_sem, a_s, a_r, rs_s, rs_r, g_s, g_r, c_s, c_r, q_s, q_r, d_s, d_r, e_s, e_r):
    x, core = lax.axis_index("dp_0"), lax.axis_index("dp_1")
    place = (lax.axis_index("feat_0"), lax.axis_index("feat_1"))
    classes = coef_ref.shape[0]

    def at(axis, step):
        return {FEAT[axis]: lax.rem(place[axis] + step, 4)}

    def feat_at(k):
        return {**at(0, k // 4), **at(1, k % 4)}

    def dp_at(k):
        return {"dp_0": lax.rem(x + k, 4)} if k else {"dp_1": 1 - core}

    def remote(src, dst, s, r, device):
        return pltpu.make_async_remote_copy(
            src_ref=src, dst_ref=dst, send_sem=s, recv_sem=r,
            device_id=device, device_id_type=pl.DeviceIdType.MESH)

    def a2a(t, c, k):
        me = place[t]
        half = CHUNK // 2

        def rows(step, part, count):
            first = (t * 4 + lax.rem(me + step, 4)) * BLOCK + c * CHUNK + part * half
            return feats.at[pl.ds(pl.multiple_of(first, half), count)]

        def to(r, part, count):
            return X.at[t, r, pl.ds(pl.multiple_of(c * CHUNK + part * half, half), count)]

        sems = (a_s.at[t, c, k], a_r.at[t, c, k])
        if k == 0:
            return remote(rows(1, 0, CHUNK), to(3, 0, CHUNK), *sems, at(t, 1))
        if k == 1:
            return remote(rows(3, 0, CHUNK), to(1, 0, CHUNK), *sems, at(t, 3))
        if k == 2:
            return remote(rows(2, 0, half), ST.at[t, c, 0], *sems, at(t, 1))
        if k == 3:
            return remote(rows(2, 1, half), ST.at[t, c, 1], *sems, at(t, 3))
        if k == 4:
            return remote(ST.at[t, c, 0], to(2, 0, half), *sems, at(t, 1))
        return remote(ST.at[t, c, 1], to(2, 1, half), *sems, at(t, 3))

    def scatter(e, t, c, k):
        axis = 1 - t
        p = place[axis]
        step = 1 if k % 2 == 0 else 3
        owner = lax.rem(p + (2 if k < 2 else step), 4)
        part = pl.ds((0, 1, 1, 0, 0, 1)[k] * 32, 32)
        dst = R1.at[e, t, c, k] if k < 2 else R2.at[e, t, c, k % 2, part]
        return remote(PL.at[e, t, c, owner, part], dst, rs_s.at[e, t, c, k], rs_r.at[e, t, c, k], at(axis, step))

    def gather(e, t, c, k):
        axis = 1 - t
        p = place[axis]
        step = 1 if k % 2 == 0 else 3
        ref = RG.at[e, t, c, p] if k < 2 else RG.at[e, t, c, lax.rem(p + 4 - step, 4), pl.ds((k - 2) * 32, 32)]
        return remote(ref, ref, g_s.at[e, t, c, k], g_r.at[e, t, c, k], at(axis, step))

    def weights(e, t, r):
        return remote(CS.at[e], CG.at[e, t, 3 - r], c_s.at[e, t, r - 1], c_r.at[e, t, r - 1], at(t, r))

    def gradients(e, t, r):
        return remote(GS.at[e, t, r], GR.at[e, t, r - 1], q_s.at[e, t, r - 1], q_r.at[e, t, r - 1], at(t, r))

    def dp_sum(e, k):
        sems = (d_s.at[e, k], d_r.at[e, k])
        if k == 0:
            return remote(DA.at[e, 1 - core], DAR.at[e], *sems, dp_at(0))
        if k < 4:
            return remote(DB.at[e, x], DB.at[e, x], *sems, dp_at(k))
        return remote(DC.at[e, core], DC.at[e, core], *sems, dp_at(0))

    def energies(k):
        mine = place[0] * 4 + place[1]
        return remote(EN.at[mine], EN.at[mine], e_s.at[k - 1], e_r.at[k - 1], feat_at(k))

    def own(t):
        first = (t * 4 + place[t]) * BLOCK
        return pltpu.make_async_copy(feats.at[pl.ds(pl.multiple_of(first, BLOCK), BLOCK)], X.at[t, 0], loc_sem.at[t])

    lane = lax.broadcasted_iota(jnp.int32, (32, 128), 1)
    low = lane < 64

    @jax.named_call
    def enter():
        barrier = pltpu.get_barrier_semaphore()
        for k in range(1, 16):
            pl.semaphore_signal(barrier, inc=1, device_id=feat_at(k), device_id_type=pl.DeviceIdType.MESH)
        for k in range(4):
            pl.semaphore_signal(barrier, inc=1, device_id=dp_at(k), device_id_type=pl.DeviceIdType.MESH)
        pl.semaphore_wait(barrier, 19)

    def pack(square):
        WIDE[:, 0:64] = square
        wide = WIDE[...]
        return jnp.concatenate([wide, pltpu.roll(wide, 96, 1)], axis=0).T[:32]

    def unpack(both):
        tall = jnp.concatenate([both, jnp.zeros((96, 128), F32)], axis=0).T
        return jnp.where(lax.broadcasted_iota(jnp.int32, (64, 128), 1) < 32, tall[:64], pltpu.roll(tall[64:], 32, 1))[:, :64]

    @jax.named_call
    def prepare():
        WIDE[...] = jnp.zeros_like(WIDE)
        POS[0:64], POS[64:96] = coef_ref[...], pack(group_ref[...])
        CS[0] = POS[...].astype(BF16)
        MOM[0:64], MOM[64:96] = coef_mom_ref[...], pack(group_mom_ref[...])
        IV[0:64] = jnp.ones((64, 128), F32)
        IV[64:96] = pack(jnp.broadcast_to(jnp.exp(-2.0 * scale_ref[...]), (64, 64)))

    @jax.named_call
    def send_weights(e):
        for t in range(2):
            for r in (2, 1, 3):
                weights(e, t, r).start()

    @jax.named_call
    def gather_weights(e):
        for t in range(2):
            for r in (1, 3, 2):
                weights(e, t, r).wait_recv()
            packed = []
            for r in range(4):
                block = CS[e] if r == 0 else CG[e, t, r - 1]
                W[t, :, r * 128:(r + 1) * 128] = block[:classes]
                packed.append(block[classes:].astype(F32))
            for i in range(2):
                a, b = packed[2 * i], packed[2 * i + 1]
                lanes = pl.ds(512 + i * 128, 128)
                W[t, 0:32, lanes] = jnp.where(low, a, pltpu.roll(b, 64, 1)).astype(BF16)
                W[t, 32:64, lanes] = jnp.where(low, pltpu.roll(a, 64, 1), b).astype(BF16)

    @jax.named_call
    def onehots():
        ids = lax.broadcasted_iota(jnp.int32, (64, 128), 0)
        for t in range(2):
            def onehot(c, _):
                for h in range(CHUNK // 128):
                    group = groups[pl.ds(((t * 4 + place[t]) * NC + c) * (CHUNK // 128) + h, 1), :]
                    for r in range(4):
                        other = lax.rem(place[t] + r, 4)
                        owner = other * 4 + place[1] if t == 0 else place[0] * 4 + other
                        hit = ids + owner * 64 == group
                        XO[t, c, 512 + r * 64:512 + (r + 1) * 64, h * 128:(h + 1) * 128] = \
                            jnp.where(hit, 1.0, 0.0).astype(BF16)
                OHT[t, c] = XO[t, c, 512:768].T
                return 0
            lax.fori_loop(0, NC, onehot, 0)

    @jax.named_call
    def send_features(c):
        for k in (2, 3, 0, 1):
            for t in range(2):
                a2a(t, c, k).start()

    @jax.named_call
    def pass_features(c):
        for k in (2, 3):
            for t in range(2):
                a2a(t, c, k).wait_recv()
                a2a(t, c, k + 2).start()

    @jax.named_call
    def wait_features(c):
        for k in (0, 1, 4, 5):
            for t in range(2):
                a2a(t, c, k).wait_recv()

    def rows_of(c):
        return pl.ds(pl.multiple_of(c * CHUNK, CHUNK), CHUNK)

    @jax.named_call
    def turn(c):
        for t in range(2):
            for r in range(4):
                XO[t, c, r * 128:(r + 1) * 128] = X[t, r, rows_of(c), :].T

    @jax.named_call
    def logits(e, c):
        for t in range(2):
            total = dot(W[t], XO[t, c])
            for o in range(4):
                PL[e, t, c, o] = total[:, o * LANES:(o + 1) * LANES]
            for k in range(4):
                scatter(e, t, c, k).start()

    @jax.named_call
    def add_passed(e, c):
        for t in range(2):
            p = place[1 - t]
            for k in range(2):
                scatter(e, t, c, k).wait_recv()
                owner = lax.rem(p + (1 if k == 0 else 3), 4)
                part = pl.ds(k * 32, 32)
                PL[e, t, c, owner, part] = PL[e, t, c, owner, part] + R1[e, t, c, k]
            for k in (4, 5):
                scatter(e, t, c, k).start()

    @jax.named_call
    def softmax(e, c):
        for t in range(2):
            p = place[1 - t]
            for k in range(2, 6):
                scatter(e, t, c, k).wait_recv()
            value = PL[e, t, c, p] + R2[e, t, c, 0] + R2[e, t, c, 1]
            first = (((t * 4 + place[t]) * NC + c) * 4 + p) * (LANES // 128)
            label = jnp.concatenate([labels[pl.ds(first + i, 1), :] for i in range(LANES // 128)], axis=1)
            shifted = value - jnp.max(value, axis=0, keepdims=True)
            scaled = jnp.exp(shifted)
            normalizer = jnp.sum(scaled, axis=0, keepdims=True)
            hit = lax.broadcasted_iota(jnp.int32, value.shape, 0) == label
            probability = scaled * (1.0 / normalizer)
            RG[e, t, c, p] = (jnp.where(hit, 1.0, 0.0) - probability).astype(BF16)
            for k in range(2):
                gather(e, t, c, k).start()
            loglik = jnp.sum(jnp.where(hit, shifted, 0.0), axis=0, keepdims=True) - jnp.log(normalizer)
            if e == 0:
                LL[t, c] = jnp.broadcast_to(loglik, (8, LANES))
            else:
                change = LL[t, c] - loglik
                for i in range(LANES // 128):
                    DIFF[...] = DIFF[...] + change[:, i * 128:(i + 1) * 128]

    @jax.named_call
    def pass_residual(e, c):
        for t in range(2):
            for k in range(2):
                gather(e, t, c, k).wait_recv()
                gather(e, t, c, k + 2).start()

    @jax.named_call
    def gradient(e, c):
        for t in range(2):
            for k in (2, 3):
                gather(e, t, c, k).wait_recv()

            rows = rows_of(c)
            res = jnp.concatenate([RG[e, t, c, o] for o in range(4)], axis=1)
            for r in (0, 2):
                two = jnp.concatenate([X[t, r, rows, :], X[t, r + 1, rows, :]], axis=1)
                ACC[t, :, r * 128:(r + 2) * 128] += dot(res, two)
            ACC[t, :, 512:768] += dot(res, OHT[t, c])

    @jax.named_call
    def ring_sum(e):
        for r in (2, 1, 3, 0):
            for t in range(2):
                GS[e, t, r, 0:classes] = ACC[t, :, r * 128:(r + 1) * 128]
                tile = 512 + (r // 2) * 128
                top, bottom = ACC[t, 0:32, tile:tile + 128], ACC[t, 32:64, tile:tile + 128]
                if r % 2 == 0:
                    GS[e, t, r, classes:] = jnp.where(low, top, pltpu.roll(bottom, 64, 1))
                else:
                    GS[e, t, r, classes:] = jnp.where(low, pltpu.roll(top, 64, 1), bottom)
                if r:
                    gradients(e, t, r).start()
        total = GS[e, 0, 0] + GS[e, 1, 0]
        for r in (1, 3, 2):
            for t in range(2):
                gradients(e, t, r).wait_recv()
                total = total + GR[e, t, r - 1]
        for h in range(2):
            DA[e, h, 0:48] = total[h * 48:(h + 1) * 48]
            DA[e, h, 48:56] = DIFF[...]

    @jax.named_call
    def core_sum(e):
        dp_sum(e, 0).start()
        dp_sum(e, 0).wait_recv()
        DB[e, x] = DA[e, core] + DAR[e]

    @jax.named_call
    def chip_sum(e):
        for k in (2, 1, 3):
            dp_sum(e, k).start()
        for k in (1, 3, 2):
            dp_sum(e, k).wait_recv()
        total = ((DB[e, 0] + DB[e, 1]) + DB[e, 2]) + DB[e, 3]
        DC[e, core] = total[0:48]
        return total[48:56]

    @jax.named_call
    def core_share(e):
        dp_sum(e, 4).start()
        dp_sum(e, 4).wait_recv()
        return jnp.concatenate([DC[e, 0], DC[e, 1]], axis=0)

    def total_gradient(e):
        ring_sum(e)
        core_sum(e)
        change = chip_sum(e)
        return core_share(e), change

    row = lax.broadcasted_iota(jnp.int32, (96, 128), 0)
    step = jnp.where(row < classes, 4.0 / math.sqrt(rows_total), 4.0 * math.sqrt(group_total / rows_total))

    @jax.named_call
    def left(e):
        def over(c, _):
            for t in range(2):
                for k in range(6):
                    if e == 0:
                        a2a(t, c, k).wait_send()
                    scatter(e, t, c, k).wait_send()
                    if k < 4:
                        gather(e, t, c, k).wait_send()
            return 0
        lax.fori_loop(0, NC, over, 0)
        for t in range(2):
            for r in range(1, 4):
                weights(e, t, r).wait_send()
                gradients(e, t, r).wait_send()
        for k in range(5):
            dp_sum(e, k).wait_send()

    def stages(s, table):
        for lag, body in table:
            c = s - lag
            pl.when(jnp.logical_and(c >= 0, c < NC))(lambda c=c, body=body: body(c))

    own(0).start()
    own(1).start()
    enter()
    for c in range(AHEAD):
        send_features(c)
    prepare()
    send_weights(0)
    DIFF[...] = jnp.zeros_like(DIFF)
    ACC[...] = jnp.zeros_like(ACC)
    onehots()
    gather_weights(0)
    own(0).wait()
    own(1).wait()

    def arrived(c):
        wait_features(c)
        turn(c)
        logits(0, c)

    def first_slot(s, _):
        stages(s, (
            (-AHEAD, send_features),
            (0, pass_features),
            (1, arrived),
            (2, lambda c: add_passed(0, c)),
            (3, lambda c: softmax(0, c)),
            (4, lambda c: pass_residual(0, c)),
            (5, lambda c: gradient(0, c)),
        ))
        return 0
    lax.fori_loop(0, NC + 5, first_slot, 0)

    grad, _ = total_gradient(0)
    half = MOM[...] + 0.5 * step * (grad - POS[...] * IV[...])
    new = POS[...] + step * half
    CS[1] = new.astype(BF16)
    send_weights(1)
    HALF[...] = half
    NEW[...] = new
    coef_out[...] = new[:classes]
    group_out[...] = unpack(new[classes:])
    left(0)

    ACC[...] = jnp.zeros_like(ACC)
    gather_weights(1)

    def over(body):
        def step_of(c, _):
            body(1, c)
            return 0
        lax.fori_loop(0, NC, step_of, 0)

    over(logits)
    over(add_passed)
    over(softmax)

    def last_slot(s, _):
        stages(s, ((0, lambda c: pass_residual(1, c)), (3, lambda c: gradient(1, c))))
        return 0
    lax.fori_loop(0, NC + 3, last_slot, 0)

    grad, change = total_gradient(1)

    @jax.named_call
    def finish():
        half, new = HALF[...], NEW[...]
        mom = half + 0.5 * step * (grad - new * IV[...])
        state = 0.5 * ((new * new - POS[...] * POS[...]) * IV[...] + (mom * mom - MOM[...] * MOM[...]))
        EN[place[0] * 4 + place[1]] = change + jnp.sum(state, axis=0, keepdims=True)
        for k in range(1, 16):
            energies(k).start()
        coef_mom_out[...] = mom[:classes]
        group_mom_out[...] = unpack(mom[classes:])
    finish()
    left(1)

    @jax.named_call
    def total_energy():
        for k in range(1, 16):
            energies(k).wait_recv()
        terms = EN[0]
        for i in range(1, 16):
            terms = terms + EN[i]
        energy_ref[...] = jnp.broadcast_to(jnp.sum(terms, axis=1, keepdims=True), (8, 128))
        for k in range(1, 16):
            energies(k).wait_send()
    total_energy()


def hand_over(*refs):
    for source, target in zip(refs[:5], refs[5:]):
        target[...] = source[0:1, 0:1] if target.shape == (1, 1) else source[...]


def per_device(
    features, labels, groups, coefficients, coef_momentum, group_effects, group_momentum, log_scale
):
    rows = labels.shape[0]
    classes = coefficients.shape[1]
    rows_total = rows * lax.axis_size(DP)
    group_total = group_effects.shape[0] * lax.axis_size(FEAT)
    vmem = pl.BlockSpec(memory_space=pltpu.VMEM)
    dma = pltpu.SemaphoreType.DMA
    shapes = [(64, 128), (64, 128), (64, 64), (64, 64)]
    results = pl.pallas_call(
        lambda *refs: kernel(rows_total, group_total, *refs),
        out_shape=[jax.ShapeDtypeStruct(s, F32) for s in shapes + [(8, 128)]],
        in_specs=[pl.BlockSpec(memory_space=pl.ANY)] + [vmem] * 7,
        out_specs=[vmem] * 5,
        scratch_shapes=[
            pltpu.VMEM((2, 4, BLOCK, 128), BF16),
            pltpu.VMEM((2, NC, 2, CHUNK // 2, 128), BF16),
            pltpu.VMEM((2, NC, 768, CHUNK), BF16),
            pltpu.VMEM((2, NC, CHUNK, 256), BF16),
            pltpu.VMEM((2, 64, 768), BF16),
            pltpu.VMEM((2, 2, NC, 4, 64, LANES), F32),
            pltpu.VMEM((2, 2, NC, 2, 32, LANES), F32),
            pltpu.VMEM((2, 2, NC, 2, 64, LANES), F32),
            pltpu.VMEM((2, 2, NC, 4, 64, LANES), BF16),
            pltpu.VMEM((2, 96, 128), BF16),
            pltpu.VMEM((2, 2, 3, 96, 128), BF16),
            pltpu.VMEM((2, 64, 768), F32),
            pltpu.VMEM((2, 2, 4, 96, 128), F32),
            pltpu.VMEM((2, 2, 3, 96, 128), F32),
            pltpu.VMEM((2, 2, 56, 128), F32),
            pltpu.VMEM((2, 56, 128), F32),
            pltpu.VMEM((2, 4, 56, 128), F32),
            pltpu.VMEM((2, 2, 48, 128), F32),
            pltpu.VMEM((16, 8, 128), F32),
            pltpu.VMEM((2, NC, 8, LANES), F32),
            pltpu.VMEM((8, 128), F32),
            pltpu.VMEM((96, 128), F32), pltpu.VMEM((96, 128), F32), pltpu.VMEM((96, 128), F32),
            pltpu.VMEM((96, 128), F32), pltpu.VMEM((96, 128), F32),
            pltpu.VMEM((64, 128), F32),
            dma((2,)),
            dma((2, NC, 6)), dma((2, NC, 6)),
            dma((2, 2, NC, 6)), dma((2, 2, NC, 6)),
            dma((2, 2, NC, 4)), dma((2, 2, NC, 4)),
            dma((2, 2, 3)), dma((2, 2, 3)),
            dma((2, 2, 3)), dma((2, 2, 3)),
            dma((2, 5)), dma((2, 5)),
            dma((15,)), dma((15,)),
        ],
        compiler_params=pltpu.CompilerParams(
            collective_id=0, has_side_effects=True, vmem_limit_bytes=58 * 2**20),
        name="leapfrog",
    )(features, labels.reshape(-1, 128), groups.reshape(-1, 128), coefficients.T, coef_momentum.T,
      group_effects, group_momentum, log_scale.reshape(1, -1))
    coef, coef_mom, group, group_mom, energy = pl.pallas_call(
        hand_over,
        out_shape=[jax.ShapeDtypeStruct(s, F32) for s in shapes + [(1, 1)]],
        in_specs=[vmem] * 5,
        out_specs=[vmem] * 5,
        name="hand_over",
    )(*results)
    return (coef.T, coef_mom.T, group, group_mom, energy[0, 0])


def solution(mesh):
    torus = Mesh(mesh.devices.reshape(4, 2, 4, 4), ("dp_0", "dp_1", "feat_0", "feat_1"))
    in_specs = (
        P(DP, FEAT),
        P(DP),
        P(DP),
        P(FEAT, None),
        P(FEAT, None),
        P(FEAT, None),
        P(FEAT, None),
        P(),
    )
    out_specs = (P(FEAT, None), P(FEAT, None), P(FEAT, None), P(FEAT, None), P())
    return jax.shard_map(
        per_device, mesh=torus, in_specs=in_specs, out_specs=out_specs, check_vma=False
    )
```

```python
import math

import jax
import jax.numpy as jnp
from jax import lax
from jax.experimental import pallas as pl
from jax.experimental.pallas import tpu as pltpu
from jax.sharding import Mesh
from jax.sharding import PartitionSpec as P

FEAT = ("feat_0", "feat_1")
DP = ("dp_0", "dp_1")

NC = 4
LANES = 1024 // NC
CHUNK = 4 * LANES
BLOCK = NC * CHUNK
AHEAD = 1
BF16, F32 = jnp.bfloat16, jnp.float32


def dot(a, b):
    return lax.dot_general(a, b, (((1,), (0,)), ((), ())), preferred_element_type=F32)


def kernel(rows_total, group_total, *refs):
    feats, sources, targets, rest = refs[0], refs[1:8], refs[8:13], refs[13:]
    body(rows_total, group_total, feats, sources, targets, *rest)


def body(rows_total, group_total, feats, sources, targets,
           labels, groups, coef_ref, coef_mom_ref, group_ref, group_mom_ref, scale_ref,
           coef_out, coef_mom_out, group_out, group_mom_out, energy_ref,
           X, ST, XO, OHT, W, PL, R1, R2, RG, CS, CG, ACC, GS, GR, DA, DAR, DB, DC, EN, LL, DIFF,
           POS, MOM, IV, HALF, NEW, WIDE,
           loc_sem, in_sem, out_sem, a_s, a_r, rs_s, rs_r, g_s, g_r, c_s, c_r, q_s, q_r, d_s, d_r, e_s, e_r):
    x, core = lax.axis_index("dp_0"), lax.axis_index("dp_1")
    place = (lax.axis_index("feat_0"), lax.axis_index("feat_1"))
    classes = coef_ref.shape[0]

    def at(axis, step):
        return {FEAT[axis]: lax.rem(place[axis] + step, 4)}

    def feat_at(k):
        return {**at(0, k // 4), **at(1, k % 4)}

    def dp_at(k):
        return {"dp_0": lax.rem(x + k, 4)} if k else {"dp_1": 1 - core}

    def remote(src, dst, s, r, device):
        return pltpu.make_async_remote_copy(
            src_ref=src, dst_ref=dst, send_sem=s, recv_sem=r,
            device_id=device, device_id_type=pl.DeviceIdType.MESH)

    def a2a(t, c, k):
        me = place[t]
        half = CHUNK // 2

        def rows(step, part, count):
            first = (t * 4 + lax.rem(me + step, 4)) * BLOCK + c * CHUNK + part * half
            return feats.at[pl.ds(pl.multiple_of(first, half), count)]

        def to(r, part, count):
            return X.at[t, r, pl.ds(pl.multiple_of(c * CHUNK + part * half, half), count)]

        sems = (a_s.at[0], a_r.at[t, c, 1 if k in (2, 3) else 0])
        if k == 0:
            return remote(rows(1, 0, CHUNK), to(3, 0, CHUNK), *sems, at(t, 1))
        if k == 1:
            return remote(rows(3, 0, CHUNK), to(1, 0, CHUNK), *sems, at(t, 3))
        if k == 2:
            return remote(rows(2, 0, half), ST.at[t, c, 0], *sems, at(t, 1))
        if k == 3:
            return remote(rows(2, 1, half), ST.at[t, c, 1], *sems, at(t, 3))
        if k == 4:
            return remote(ST.at[t, c, 0], to(2, 0, half), *sems, at(t, 1))
        return remote(ST.at[t, c, 1], to(2, 1, half), *sems, at(t, 3))

    def scatter(e, t, c, k):
        axis = 1 - t
        p = place[axis]
        step = 1 if k % 2 == 0 else 3
        owner = lax.rem(p + (2 if k < 2 else step), 4)
        part = pl.ds((0, 1, 1, 0, 0, 1)[k] * 32, 32)
        dst = R1.at[e, t, c, k] if k < 2 else R2.at[e, t, c, k % 2, part]
        return remote(PL.at[e, t, c, owner, part], dst, rs_s.at[e], rs_r.at[e, t, c, 0 if k < 2 else 1], at(axis, step))

    def gather(e, t, c, k):
        axis = 1 - t
        p = place[axis]
        step = 1 if k % 2 == 0 else 3
        ref = RG.at[e, t, c, p] if k < 2 else RG.at[e, t, c, lax.rem(p + 4 - step, 4), pl.ds((k - 2) * 32, 32)]
        return remote(ref, ref, g_s.at[e], g_r.at[e, t, c, k // 2], at(axis, step))

    def weights(e, t, r):
        return remote(CS.at[e], CG.at[e, t, 3 - r], c_s.at[e], c_r.at[e, t], at(t, r))

    def gradients(e, t, r):
        return remote(GS.at[e, t, r], GR.at[e, t, r - 1], q_s.at[e], q_r.at[e, t], at(t, r))

    def dp_sum(e, k):
        sems = (d_s.at[e], d_r.at[e, (0, 1, 1, 1, 2)[k]])
        if k == 0:
            return remote(DA.at[e, 1 - core], DAR.at[e], *sems, dp_at(0))
        if k < 4:
            return remote(DB.at[e, x], DB.at[e, x], *sems, dp_at(k))
        return remote(DC.at[e, core], DC.at[e, core], *sems, dp_at(0))

    def energies(k):
        mine = place[0] * 4 + place[1]
        return remote(EN.at[mine], EN.at[mine], e_s.at[0], e_r.at[0], feat_at(k))

    def bytes_of(ref, sem):
        pltpu.make_async_copy(ref, ref, sem).wait()

    def own(t):
        first = (t * 4 + place[t]) * BLOCK
        return pltpu.make_async_copy(feats.at[pl.ds(pl.multiple_of(first, BLOCK), BLOCK)], X.at[t, 0], loc_sem.at[t])

    def fetch(i):
        local = (labels, groups, coef_ref, coef_mom_ref, group_ref, group_mom_ref, scale_ref)[i]
        return pltpu.make_async_copy(sources[i], local, in_sem.at[i])

    def store(i):
        local = (coef_out, coef_mom_out, group_out, group_mom_out, energy_ref)[i]
        return pltpu.make_async_copy(local, targets[i], out_sem.at[i])

    lane = lax.broadcasted_iota(jnp.int32, (32, 128), 1)
    low = lane < 64

    barrier = pltpu.get_barrier_semaphore()

    @jax.named_call
    def enter():
        peers = [at(axis, k) for axis in range(2) for k in range(1, 4)] + [dp_at(k) for k in range(4)]
        for peer in peers:
            pl.semaphore_signal(barrier, inc=1, device_id=peer, device_id_type=pl.DeviceIdType.MESH)
        for i in (2, 4, 3, 5, 6, 0, 1):
            fetch(i).start()

    @jax.named_call
    def met():
        pl.semaphore_wait(barrier, 10)

    def pack(square):
        WIDE[:, 0:64] = square
        wide = WIDE[...]
        return jnp.concatenate([wide, pltpu.roll(wide, 96, 1)], axis=0).T[:32]

    def unpack(both):
        tall = jnp.concatenate([both, jnp.zeros((96, 128), F32)], axis=0).T
        return jnp.where(lax.broadcasted_iota(jnp.int32, (64, 128), 1) < 32, tall[:64], pltpu.roll(tall[64:], 32, 1))[:, :64]

    @jax.named_call
    def prepare():
        WIDE[...] = jnp.zeros_like(WIDE)
        DIFF[...] = jnp.zeros_like(DIFF)
        ACC[...] = jnp.zeros_like(ACC)
        for i in (2, 4, 3, 5, 6):
            fetch(i).wait()
        POS[0:64], POS[64:96] = coef_ref[...], pack(group_ref[...])
        CS[0] = POS[...].astype(BF16)
        MOM[0:64], MOM[64:96] = coef_mom_ref[...], pack(group_mom_ref[...])
        IV[0:64] = jnp.ones((64, 128), F32)
        IV[64:96] = pack(jnp.broadcast_to(jnp.exp(-2.0 * scale_ref[...]), (64, 64)))

    @jax.named_call
    def send_weights(e):
        for t in range(2):
            for r in (2, 1, 3):
                weights(e, t, r).start()

    @jax.named_call
    def gather_weights(e):
        for t in range(2):
            bytes_of(CG.at[e, t], c_r.at[e, t])
            packed = []
            for r in range(4):
                block = CS[e] if r == 0 else CG[e, t, r - 1]
                W[t, :, r * 128:(r + 1) * 128] = block[:classes]
                packed.append(block[classes:].astype(F32))
            for i in range(2):
                a, b = packed[2 * i], packed[2 * i + 1]
                lanes = pl.ds(512 + i * 128, 128)
                W[t, 0:32, lanes] = jnp.where(low, a, pltpu.roll(b, 64, 1)).astype(BF16)
                W[t, 32:64, lanes] = jnp.where(low, pltpu.roll(a, 64, 1), b).astype(BF16)

    @jax.named_call
    def onehots():
        ids = lax.broadcasted_iota(jnp.int32, (64, 128), 0)
        for t in range(2):
            def onehot(c, _):
                for h in range(CHUNK // 128):
                    group = groups[pl.ds(((t * 4 + place[t]) * NC + c) * (CHUNK // 128) + h, 1), :]
                    for r in range(4):
                        other = lax.rem(place[t] + r, 4)
                        owner = other * 4 + place[1] if t == 0 else place[0] * 4 + other
                        hit = ids + owner * 64 == group
                        XO[t, c, 512 + r * 64:512 + (r + 1) * 64, h * 128:(h + 1) * 128] = \
                            jnp.where(hit, 1.0, 0.0).astype(BF16)
                OHT[t, c] = XO[t, c, 512:768].T
                return 0
            lax.fori_loop(0, NC, onehot, 0)

    @jax.named_call
    def send_features(c):
        for k in (2, 3, 0, 1):
            for t in range(2):
                a2a(t, c, k).start()

    @jax.named_call
    def pass_features(c):
        for t in range(2):
            bytes_of(ST.at[t, c], a_r.at[t, c, 1])
            a2a(t, c, 4).start()
            a2a(t, c, 5).start()

    @jax.named_call
    def wait_features(c):
        for t in range(2):
            bytes_of(X.at[t, pl.ds(1, 3), rows_of(c)], a_r.at[t, c, 0])

    def rows_of(c):
        return pl.ds(pl.multiple_of(c * CHUNK, CHUNK), CHUNK)

    @jax.named_call
    def turn(c):
        for t in range(2):
            for r in range(4):
                XO[t, c, r * 128:(r + 1) * 128] = X[t, r, rows_of(c), :].T

    @jax.named_call
    def logits(e, c):
        for t in range(2):
            total = dot(W[t], XO[t, c])
            for o in range(4):
                PL[e, t, c, o] = total[:, o * LANES:(o + 1) * LANES]
            for k in range(4):
                scatter(e, t, c, k).start()

    @jax.named_call
    def add_passed(e, c):
        for t in range(2):
            p = place[1 - t]
            bytes_of(R1.at[e, t, c], rs_r.at[e, t, c, 0])
            for k in range(2):
                owner = lax.rem(p + (1 if k == 0 else 3), 4)
                part = pl.ds(k * 32, 32)
                PL[e, t, c, owner, part] = PL[e, t, c, owner, part] + R1[e, t, c, k]
            for k in (4, 5):
                scatter(e, t, c, k).start()

    @jax.named_call
    def softmax(e, c):
        for t in range(2):
            p = place[1 - t]
            bytes_of(R2.at[e, t, c], rs_r.at[e, t, c, 1])
            value = PL[e, t, c, p] + R2[e, t, c, 0] + R2[e, t, c, 1]
            first = (((t * 4 + place[t]) * NC + c) * 4 + p) * (LANES // 128)
            label = jnp.concatenate([labels[pl.ds(first + i, 1), :] for i in range(LANES // 128)], axis=1)
            shifted = value - jnp.max(value, axis=0, keepdims=True)
            scaled = jnp.exp(shifted)
            normalizer = jnp.sum(scaled, axis=0, keepdims=True)
            hit = lax.broadcasted_iota(jnp.int32, value.shape, 0) == label
            probability = scaled * (1.0 / normalizer)
            RG[e, t, c, p] = (jnp.where(hit, 1.0, 0.0) - probability).astype(BF16)
            for k in range(2):
                gather(e, t, c, k).start()
            loglik = jnp.sum(jnp.where(hit, shifted, 0.0), axis=0, keepdims=True) - jnp.log(normalizer)
            if e == 0:
                LL[t, c] = jnp.broadcast_to(loglik, (8, LANES))
            else:
                change = LL[t, c] - loglik
                for i in range(LANES // 128):
                    DIFF[...] = DIFF[...] + change[:, i * 128:(i + 1) * 128]

    @jax.named_call
    def pass_residual(e, c):
        for t in range(2):
            bytes_of(RG.at[e, t, c, pl.ds(0, 2)], g_r.at[e, t, c, 0])
            gather(e, t, c, 2).start()
            gather(e, t, c, 3).start()

    @jax.named_call
    def gradient(e, c):
        for t in range(2):
            bytes_of(RG.at[e, t, c, 0], g_r.at[e, t, c, 1])

            rows = rows_of(c)
            res = jnp.concatenate([RG[e, t, c, o] for o in range(4)], axis=1)
            for r in (0, 2):
                two = jnp.concatenate([X[t, r, rows, :], X[t, r + 1, rows, :]], axis=1)
                ACC[t, :, r * 128:(r + 2) * 128] += dot(res, two)
            ACC[t, :, 512:768] += dot(res, OHT[t, c])

    @jax.named_call
    def ring_sum(e):
        for r in (2, 1, 3, 0):
            for t in range(2):
                GS[e, t, r, 0:classes] = ACC[t, :, r * 128:(r + 1) * 128]
                tile = 512 + (r // 2) * 128
                top, bottom = ACC[t, 0:32, tile:tile + 128], ACC[t, 32:64, tile:tile + 128]
                if r % 2 == 0:
                    GS[e, t, r, classes:] = jnp.where(low, top, pltpu.roll(bottom, 64, 1))
                else:
                    GS[e, t, r, classes:] = jnp.where(low, pltpu.roll(top, 64, 1), bottom)
                if r:
                    gradients(e, t, r).start()
        total = GS[e, 0, 0] + GS[e, 1, 0]
        for t in range(2):
            bytes_of(GR.at[e, t], q_r.at[e, t])
            for r in range(3):
                total = total + GR[e, t, r]
        for h in range(2):
            DA[e, h, 0:48] = total[h * 48:(h + 1) * 48]
            DA[e, h, 48:56] = DIFF[...]

    @jax.named_call
    def core_sum(e):
        dp_sum(e, 0).start()
        dp_sum(e, 0).wait_recv()
        DB[e, x] = DA[e, core] + DAR[e]

    @jax.named_call
    def chip_sum(e):
        for k in (2, 1, 3):
            dp_sum(e, k).start()
        bytes_of(DB.at[e, pl.ds(0, 3)], d_r.at[e, 1])
        total = ((DB[e, 0] + DB[e, 1]) + DB[e, 2]) + DB[e, 3]
        DC[e, core] = total[0:48]
        return total[48:56]

    @jax.named_call
    def core_share(e):
        dp_sum(e, 4).start()
        dp_sum(e, 4).wait_recv()
        return jnp.concatenate([DC[e, 0], DC[e, 1]], axis=0)

    def total_gradient(e):
        ring_sum(e)
        core_sum(e)
        change = chip_sum(e)
        return core_share(e), change

    row = lax.broadcasted_iota(jnp.int32, (96, 128), 0)
    step = jnp.where(row < classes, 4.0 / math.sqrt(rows_total), 4.0 * math.sqrt(group_total / rows_total))

    @jax.named_call
    def left(e):
        if e == 0:
            bytes_of(X, a_s.at[0])
        most = pl.ds(0, NC * 3 // 4)
        bytes_of(PL.at[e, :, most], rs_s.at[e])
        bytes_of(RG.at[e, :, most], g_s.at[e])
        bytes_of(CG.at[e], c_s.at[e])
        bytes_of(GR.at[e], q_s.at[e])
        bytes_of(X.at[0, 0, pl.ds(0, 2 * (4 * 56 + 48))], d_s.at[e])

    def stages(s, table):
        for lag, body in table:
            c = s - lag
            pl.when(jnp.logical_and(c >= 0, c < NC))(lambda c=c, body=body: body(c))

    enter()
    prepare()
    met()
    send_weights(0)
    for c in range(AHEAD):
        send_features(c)
    own(0).start()
    own(1).start()
    fetch(0).wait()
    fetch(1).wait()
    onehots()
    gather_weights(0)
    own(0).wait()
    own(1).wait()

    def arrived(c):
        wait_features(c)
        turn(c)
        logits(0, c)

    def first_slot(s, _):
        stages(s, (
            (-AHEAD, send_features),
            (0, pass_features),
            (1, arrived),
            (2, lambda c: add_passed(0, c)),
            (3, lambda c: softmax(0, c)),
            (4, lambda c: pass_residual(0, c)),
            (5, lambda c: gradient(0, c)),
        ))
        return 0
    lax.fori_loop(0, NC + 5, first_slot, 0)

    grad, _ = total_gradient(0)
    half = MOM[...] + 0.5 * step * (grad - POS[...] * IV[...])
    new = POS[...] + step * half
    CS[1] = new.astype(BF16)
    send_weights(1)
    HALF[...] = half
    NEW[...] = new
    coef_out[...] = new[:classes]
    group_out[...] = unpack(new[classes:])
    store(0).start()
    store(2).start()
    left(0)

    ACC[...] = jnp.zeros_like(ACC)
    gather_weights(1)

    def over(body):
        def step_of(c, _):
            body(1, c)
            return 0
        lax.fori_loop(0, NC, step_of, 0)

    over(logits)
    over(add_passed)
    over(softmax)

    def last_slot(s, _):
        stages(s, ((0, lambda c: pass_residual(1, c)), (3, lambda c: gradient(1, c))))
        return 0
    lax.fori_loop(0, NC + 3, last_slot, 0)

    grad, change = total_gradient(1)

    @jax.named_call
    def finish():
        half, new = HALF[...], NEW[...]
        mom = half + 0.5 * step * (grad - new * IV[...])
        state = 0.5 * ((new * new - POS[...] * POS[...]) * IV[...] + (mom * mom - MOM[...] * MOM[...]))
        EN[place[0] * 4 + place[1]] = change + jnp.sum(state, axis=0, keepdims=True)
        for k in range(1, 16):
            energies(k).start()
        coef_mom_out[...] = mom[:classes]
        group_mom_out[...] = unpack(mom[classes:])
        store(1).start()
        store(3).start()
    finish()
    left(1)
    for i in range(4):
        store(i).wait()

    @jax.named_call
    def total_energy():
        bytes_of(EN.at[pl.ds(0, 15)], e_r.at[0])
        terms = EN[0]
        for i in range(1, 16):
            terms = terms + EN[i]
        energy_ref[...] = jnp.broadcast_to(jnp.sum(terms, axis=1, keepdims=True), (8, 128))
        store(4).start()
        bytes_of(EN.at[pl.ds(0, 15)], e_s.at[0])
        store(4).wait()
    total_energy()


def hand_over(*refs):
    for source, target in zip(refs[:5], refs[5:]):
        target[...] = source[0:1, 0:1] if target.shape == (1, 1) else source[...]


def per_device(
    features, labels, groups, coefficients, coef_momentum, group_effects, group_momentum, log_scale
):
    rows = labels.shape[0]
    classes = coefficients.shape[1]
    rows_total = rows * lax.axis_size(DP)
    group_total = group_effects.shape[0] * lax.axis_size(FEAT)
    vmem = pl.BlockSpec(memory_space=pltpu.VMEM)
    dma = pltpu.SemaphoreType.DMA
    shapes = [(64, 128), (64, 128), (64, 64), (64, 64)]
    results = pl.pallas_call(
        lambda *refs: kernel(rows_total, group_total, *refs),
        out_shape=[jax.ShapeDtypeStruct(s, F32) for s in shapes + [(8, 128)]],
        in_specs=[pl.BlockSpec(memory_space=pl.ANY)] * 8,
        out_specs=[pl.BlockSpec(memory_space=pl.ANY)] * 5,
        scratch_shapes=[
            pltpu.VMEM((rows // 128, 128), jnp.int32), pltpu.VMEM((rows // 128, 128), jnp.int32),
            pltpu.VMEM((64, 128), F32), pltpu.VMEM((64, 128), F32),
            pltpu.VMEM((64, 64), F32), pltpu.VMEM((64, 64), F32), pltpu.VMEM((1, 64), F32),
            pltpu.VMEM((64, 128), F32), pltpu.VMEM((64, 128), F32),
            pltpu.VMEM((64, 64), F32), pltpu.VMEM((64, 64), F32), pltpu.VMEM((8, 128), F32),
            pltpu.VMEM((2, 4, BLOCK, 128), BF16),
            pltpu.VMEM((2, NC, 2, CHUNK // 2, 128), BF16),
            pltpu.VMEM((2, NC, 768, CHUNK), BF16),
            pltpu.VMEM((2, NC, CHUNK, 256), BF16),
            pltpu.VMEM((2, 64, 768), BF16),
            pltpu.VMEM((2, 2, NC, 4, 64, LANES), F32),
            pltpu.VMEM((2, 2, NC, 2, 32, LANES), F32),
            pltpu.VMEM((2, 2, NC, 2, 64, LANES), F32),
            pltpu.VMEM((2, 2, NC, 4, 64, LANES), BF16),
            pltpu.VMEM((2, 96, 128), BF16),
            pltpu.VMEM((2, 2, 3, 96, 128), BF16),
            pltpu.VMEM((2, 64, 768), F32),
            pltpu.VMEM((2, 2, 4, 96, 128), F32),
            pltpu.VMEM((2, 2, 3, 96, 128), F32),
            pltpu.VMEM((2, 2, 56, 128), F32),
            pltpu.VMEM((2, 56, 128), F32),
            pltpu.VMEM((2, 4, 56, 128), F32),
            pltpu.VMEM((2, 2, 48, 128), F32),
            pltpu.VMEM((16, 8, 128), F32),
            pltpu.VMEM((2, NC, 8, LANES), F32),
            pltpu.VMEM((8, 128), F32),
            pltpu.VMEM((96, 128), F32), pltpu.VMEM((96, 128), F32), pltpu.VMEM((96, 128), F32),
            pltpu.VMEM((96, 128), F32), pltpu.VMEM((96, 128), F32),
            pltpu.VMEM((64, 128), F32),
            dma((2,)), dma((7,)), dma((5,)),
            dma((1,)), dma((2, NC, 2)),
            dma((2,)), dma((2, 2, NC, 2)),
            dma((2,)), dma((2, 2, NC, 2)),
            dma((2,)), dma((2, 2)),
            dma((2,)), dma((2, 2)),
            dma((2,)), dma((2, 3)),
            dma((1,)), dma((1,)),
        ],
        compiler_params=pltpu.CompilerParams(
            collective_id=0, has_side_effects=True, vmem_limit_bytes=58 * 2**20),
        name="leapfrog",
    )(features, labels.reshape(-1, 128), groups.reshape(-1, 128), coefficients.T, coef_momentum.T,
      group_effects, group_momentum, log_scale.reshape(1, -1))
    coef, coef_mom, group, group_mom, energy = pl.pallas_call(
        hand_over,
        out_shape=[jax.ShapeDtypeStruct(s, F32) for s in shapes + [(1, 1)]],
        in_specs=[vmem] * 5,
        out_specs=[vmem] * 5,
        name="hand_over",
    )(*results)
    return (coef.T, coef_mom.T, group, group_mom, energy[0, 0])


def solution(mesh):
    torus = Mesh(mesh.devices.reshape(4, 2, 4, 4), ("dp_0", "dp_1", "feat_0", "feat_1"))
    in_specs = (
        P(DP, FEAT),
        P(DP),
        P(DP),
        P(FEAT, None),
        P(FEAT, None),
        P(FEAT, None),
        P(FEAT, None),
        P(),
    )
    out_specs = (P(FEAT, None), P(FEAT, None), P(FEAT, None), P(FEAT, None), P())
    return jax.shard_map(
        per_device, mesh=torus, in_specs=in_specs, out_specs=out_specs, check_vma=False
    )
```

```python
import math

import jax
import jax.numpy as jnp
from jax import lax
from jax.experimental import pallas as pl
from jax.experimental.pallas import tpu as pltpu
from jax.sharding import Mesh
from jax.sharding import PartitionSpec as P

FEAT = ("feat_0", "feat_1")
DP = ("dp_0", "dp_1")

UNITS = 8
UNIT = 4 * 128
BLOCK = UNITS * UNIT
SIZES = (2, 2, 2, 1, 1)
NC = len(SIZES)
CHUNKS = tuple((sum(SIZES[:c]), SIZES[c]) for c in range(NC))
DIRECT_SUMS = ((0, NC - 1), (1, NC - 1))
DIRECT_RESIDUALS = ((0, NC - 1),)
BF16, F32 = jnp.bfloat16, jnp.float32


def dot(a, b):
    return lax.dot_general(a, b, (((1,), (0,)), ((), ())), preferred_element_type=F32)


def kernel(rows_total, group_total, *refs):
    feats, sources, targets, rest = refs[0], refs[1:8], refs[8:13], refs[13:]
    body(rows_total, group_total, feats, sources, targets, *rest)


def body(rows_total, group_total, feats, sources, targets,
           labels, groups, coef_ref, coef_mom_ref, group_ref, group_mom_ref, scale_ref,
           coef_out, coef_mom_out, group_out, group_mom_out, energy_ref,
           X, ST, XO, OHT, W, PL, R1, R2, RG, CS, CG, ACC, GS, GC, GR, DB, DC, EN, LL, DIFF,
           POS, MOM, IV, STEP, HALF, NEW, WIDE,
           loc_sem, in_sem, out_sem, a_s, a_r, rs_s, rs_r, g_s, g_r, c_s, c_r, h_s, h_r, q_s, q_r, d_s, d_r, e_s, e_r):
    x, core = lax.axis_index("dp_0"), lax.axis_index("dp_1")
    place = (lax.axis_index("feat_0"), lax.axis_index("feat_1"))
    classes = coef_ref.shape[0]

    def at(axis, step):
        return {FEAT[axis]: lax.rem(place[axis] + step, 4)}

    def feat_at(k):
        return {**at(0, k // 4), **at(1, k % 4)}

    def dp_at(k):
        return {"dp_0": lax.rem(x + k, 4)} if k else {"dp_1": 1 - core}

    def remote(src, dst, s, r, device):
        return pltpu.make_async_remote_copy(
            src_ref=src, dst_ref=dst, send_sem=s, recv_sem=r,
            device_id=device, device_id_type=pl.DeviceIdType.MESH)

    def a2a(t, c, k):
        me = place[t]
        unit, units = CHUNKS[c]
        chunk, half = units * UNIT, units * UNIT // 2

        def rows(step, part, count):
            first = (t * 4 + lax.rem(me + step, 4)) * BLOCK + unit * UNIT + part * half
            return feats.at[pl.ds(pl.multiple_of(first, UNIT // 2), count)]

        def to(r, part, count):
            return X.at[t, r, pl.ds(unit * UNIT + part * half, count)]

        def staged(part):
            return ST.at[t, part, pl.ds(unit * UNIT // 2, half)]

        sems = (a_s.at[0], a_r.at[t, c, 1 if k in (2, 3) else 0])
        if k == 0:
            return remote(rows(1, 0, chunk), to(3, 0, chunk), *sems, at(t, 1))
        if k == 1:
            return remote(rows(3, 0, chunk), to(1, 0, chunk), *sems, at(t, 3))
        if k == 2:
            return remote(rows(2, 0, half), staged(0), *sems, at(t, 1))
        if k == 3:
            return remote(rows(2, 1, half), staged(1), *sems, at(t, 3))
        if k == 4:
            return remote(staged(0), to(2, 0, half), *sems, at(t, 1))
        return remote(staged(1), to(2, 1, half), *sems, at(t, 3))

    def scatter(e, t, c, k):
        axis = 1 - t
        p = place[axis]
        step = 1 if k % 2 == 0 else 3
        if k < 2 and (e, c) in DIRECT_SUMS:
            step = 2
        owner = lax.rem(p + (2 if k < 2 else step), 4)
        part = pl.ds((0, 1, 1, 0, 0, 1)[k] * 32, 32)
        units = pl.ds(*CHUNKS[c])
        dst = R1.at[e, t, k, units] if k < 2 else R2.at[e, t, k % 2, units, part]
        return remote(PL.at[e, t, units, owner, part], dst, rs_s.at[e], rs_r.at[e, t, c, 0 if k < 2 else 1], at(axis, step))

    def gather(e, t, c, k):
        axis = 1 - t
        p = place[axis]
        step = 2 if k == 4 else 1 if k % 2 == 0 else 3
        units = pl.ds(*CHUNKS[c])
        ref = RG.at[e, t, units, p]
        if k in (2, 3):
            ref = RG.at[e, t, units, lax.rem(p + 4 - step, 4), pl.ds((k - 2) * 32, 32)]
        return remote(ref, ref, g_s.at[e], g_r.at[e, t, c, 0 if k < 2 else 1], at(axis, step))

    def both(device, other):
        return {**device, "dp_1": 1 - core} if other else device

    def weights(e, t, r, other):
        if e == 0:
            return remote(CS.at[0, other], CG.at[0, t, 3 - r, other], c_s.at[0], c_r.at[0, t], at(t, r))
        half = CS.at[e, core]
        return remote(half, CG.at[e, t, 3 - r, core], c_s.at[e], c_r.at[e, t], both(at(t, r), other))

    def weights_across(e):
        half = CS.at[e, core]
        return remote(half, half, h_s.at[e, 0], h_r.at[e, 0], dp_at(0))

    def gradients_across(e):
        return remote(GS.at[e, 1 - core], GC.at[e], h_s.at[e, 1], h_r.at[e, 1], dp_at(0))

    def gradients(e, t, r):
        return remote(GS.at[e, core, t, r], GR.at[e, t, r - 1], q_s.at[e], q_r.at[e, t], at(t, r))

    def chips(e, k):
        return remote(DB.at[e, x], DB.at[e, x], d_s.at[e], d_r.at[e], dp_at(k))

    def totals_across(e):
        return remote(DC.at[e, core], DC.at[e, core], h_s.at[e, 2], h_r.at[e, 2], dp_at(0))

    def energies(k, other):
        mine = EN.at[core * 16 + place[0] * 4 + place[1]]
        return remote(mine, mine, e_s.at[0], e_r.at[0], both(feat_at(k), other))

    def bytes_of(ref, sem):
        pltpu.make_async_copy(ref, ref, sem).wait()

    def own(t):
        first = (t * 4 + place[t]) * BLOCK
        return pltpu.make_async_copy(feats.at[pl.ds(pl.multiple_of(first, BLOCK), BLOCK)], X.at[t, 0], loc_sem.at[t])

    def fetch(i):
        local = (labels, groups, coef_ref, coef_mom_ref, group_ref, group_mom_ref, scale_ref)[i]
        return pltpu.make_async_copy(sources[i], local, in_sem.at[i])

    def store(i):
        local = (coef_out, coef_mom_out, group_out, group_mom_out, energy_ref)[i]
        return pltpu.make_async_copy(local, targets[i], out_sem.at[i])

    lane = lax.broadcasted_iota(jnp.int32, (32, 128), 1)
    low = lane < 64

    barrier = pltpu.get_barrier_semaphore()

    @jax.named_call
    def enter():
        peers = [at(axis, k) for axis in range(2) for k in range(1, 4)] + [dp_at(k) for k in range(4)]
        for peer in peers:
            pl.semaphore_signal(barrier, inc=1, device_id=peer, device_id_type=pl.DeviceIdType.MESH)
        for i in (2, 4, 3, 5, 6, 0, 1):
            fetch(i).start()

    @jax.named_call
    def met():
        pl.semaphore_wait(barrier, 10)

    def pack(square):
        WIDE[:, 0:64] = square
        wide = WIDE[...]
        return jnp.concatenate([wide, pltpu.roll(wide, 96, 1)], axis=0).T[:32]

    def unpack(both):
        tall = jnp.concatenate([both, jnp.zeros((96, 128), F32)], axis=0).T
        return jnp.where(lax.broadcasted_iota(jnp.int32, (64, 128), 1) < 32, tall[:64], pltpu.roll(tall[64:], 32, 1))[:, :64]

    def keep(ref, top, bottom):
        ref[0] = top[0:48]
        ref[1, 0:16], ref[1, 16:48] = top[48:64], bottom

    def kept(first, second):
        return jnp.concatenate([first, second[0:16]], axis=0), second[16:48]

    @jax.named_call
    def prepare():
        WIDE[...] = jnp.zeros_like(WIDE)
        DIFF[...] = jnp.zeros_like(DIFF)
        ACC[...] = jnp.zeros_like(ACC)
        for i in (2, 4, 3, 5, 6):
            fetch(i).wait()
        keep(POS, coef_ref[...], pack(group_ref[...]))
        CS[0] = POS[...].astype(BF16)
        keep(MOM, coef_mom_ref[...], pack(group_mom_ref[...]))
        keep(IV, jnp.ones((64, 128), F32), pack(jnp.broadcast_to(jnp.exp(-2.0 * scale_ref[...]), (64, 64))))
        row = lax.broadcasted_iota(jnp.int32, (48, 128), 0)
        small, large = 4.0 / math.sqrt(rows_total), 4.0 * math.sqrt(group_total / rows_total)
        STEP[0] = jnp.full((48, 128), small, F32)
        STEP[1] = jnp.where(row < classes - 48, small, large)

    @jax.named_call
    def send_weights(e):
        if e:
            weights_across(e).start()
        for t in range(2):
            for r in (2, 1, 3):
                for other in range(2):
                    weights(e, t, r, other).start()

    @jax.named_call
    def gather_weights(e):
        if e:
            weights_across(e).wait_recv()
        for t in range(2):
            bytes_of(CG.at[e, t], c_r.at[e, t])
            packed = []
            for r in range(4):
                first, second = (CS[e, 0], CS[e, 1]) if r == 0 else (CG[e, t, r - 1, 0], CG[e, t, r - 1, 1])
                W[t, 0:48, r * 128:(r + 1) * 128] = first
                W[t, 48:64, r * 128:(r + 1) * 128] = second[0:16]
                packed.append(second[16:48].astype(F32))
            for i in range(2):
                a, b = packed[2 * i], packed[2 * i + 1]
                lanes = pl.ds(512 + i * 128, 128)
                W[t, 0:32, lanes] = jnp.where(low, a, pltpu.roll(b, 64, 1)).astype(BF16)
                W[t, 32:64, lanes] = jnp.where(low, pltpu.roll(a, 64, 1), b).astype(BF16)

    @jax.named_call
    def onehots():
        ids = lax.broadcasted_iota(jnp.int32, (64, 128), 0)
        for t in range(2):
            def onehot(u, _):
                for h in range(4):
                    group = groups[pl.ds(((t * 4 + place[t]) * UNITS + u) * 4 + h, 1), :]
                    for r in range(4):
                        other = lax.rem(place[t] + r, 4)
                        owner = other * 4 + place[1] if t == 0 else place[0] * 4 + other
                        hit = ids + owner * 64 == group
                        XO[t, u, 512 + r * 64:512 + (r + 1) * 64, h * 128:(h + 1) * 128] = \
                            jnp.where(hit, 1.0, 0.0).astype(BF16)
                OHT[t, u] = XO[t, u, 512:768].T
                return 0
            lax.fori_loop(0, UNITS, onehot, 0)

    @jax.named_call
    def send_features(c):
        for k in (2, 3, 0, 1):
            for t in range(2):
                a2a(t, c, k).start()

    @jax.named_call
    def pass_features(c):
        for t in range(2):
            bytes_of(X.at[t, 0, pl.ds(0, CHUNKS[c][1] * UNIT)], a_r.at[t, c, 1])
            a2a(t, c, 4).start()
            a2a(t, c, 5).start()

    @jax.named_call
    def wait_features(c):
        for t in range(2):
            bytes_of(X.at[t, pl.ds(1, 3), pl.ds(0, CHUNKS[c][1] * UNIT)], a_r.at[t, c, 0])

    def units_of(c):
        return range(CHUNKS[c][0], sum(CHUNKS[c]))

    def rows_of(u):
        return slice(u * UNIT, (u + 1) * UNIT)

    @jax.named_call
    def turn(c):
        for t in range(2):
            for u in units_of(c):
                for r in range(4):
                    XO[t, u, r * 128:(r + 1) * 128] = X[t, r, rows_of(u), :].T

    @jax.named_call
    def logits(e, c):
        for t in range(2):
            for u in units_of(c):
                total = dot(W[t], XO[t, u])
                for o in range(4):
                    PL[e, t, u, o] = total[:, o * 128:(o + 1) * 128]
            for k in range(6 if (e, c) in DIRECT_SUMS else 4):
                scatter(e, t, c, k).start()

    @jax.named_call
    def add_passed(e, c):
        if (e, c) in DIRECT_SUMS:
            return
        for t in range(2):
            p = place[1 - t]
            bytes_of(R1.at[e, t, :, pl.ds(*CHUNKS[c])], rs_r.at[e, t, c, 0])
            for k in range(2):
                owner = lax.rem(p + (1 if k == 0 else 3), 4)
                part = pl.ds(k * 32, 32)
                for u in units_of(c):
                    PL[e, t, u, owner, part] = PL[e, t, u, owner, part] + R1[e, t, k, u]
            for k in (4, 5):
                scatter(e, t, c, k).start()

    @jax.named_call
    def softmax(e, c):
        for t in range(2):
            p = place[1 - t]
            bytes_of(R2.at[e, t, :, pl.ds(*CHUNKS[c])], rs_r.at[e, t, c, 1])
            if (e, c) in DIRECT_SUMS:
                bytes_of(R1.at[e, t, :, pl.ds(*CHUNKS[c])], rs_r.at[e, t, c, 0])
            for u in units_of(c):
                value = PL[e, t, u, p] + R2[e, t, 0, u] + R2[e, t, 1, u]
                if (e, c) in DIRECT_SUMS:
                    value = value + jnp.concatenate([R1[e, t, 0, u], R1[e, t, 1, u]], axis=0)
                label = labels[pl.ds(((t * 4 + place[t]) * UNITS + u) * 4 + p, 1), :]
                shifted = value - jnp.max(value, axis=0, keepdims=True)
                scaled = jnp.exp(shifted)
                normalizer = jnp.sum(scaled, axis=0, keepdims=True)
                hit = lax.broadcasted_iota(jnp.int32, value.shape, 0) == label
                probability = scaled * (1.0 / normalizer)
                RG[e, t, u, p] = (jnp.where(hit, 1.0, 0.0) - probability).astype(BF16)
                loglik = jnp.sum(jnp.where(hit, shifted, 0.0), axis=0, keepdims=True) - jnp.log(normalizer)
                if e == 0:
                    LL[t, u] = jnp.broadcast_to(loglik, (8, 128))
                else:
                    DIFF[...] = DIFF[...] + (LL[t, u] - loglik)
            for k in (4, 0, 1) if (e, c) in DIRECT_RESIDUALS else (0, 1):
                gather(e, t, c, k).start()

    def accumulate(e, t, c, steps):
        owners = [lax.rem(place[1 - t] + step, 4) for step in steps]
        runs = [(u, o) for u in units_of(c) for o in owners]
        res = jnp.concatenate([RG[e, t, u, o] for u, o in runs], axis=1)
        rows = [pl.ds(pl.multiple_of(u * UNIT + o * 128, 128), 128) for u, o in runs]
        for r in (0, 2):
            two = jnp.concatenate(
                [jnp.concatenate([X[t, r, row, :], X[t, r + 1, row, :]], axis=1) for row in rows], axis=0)
            ACC[t, :, r * 128:(r + 2) * 128] += dot(res, two)
        onehot = jnp.concatenate([OHT[t, u, pl.ds(pl.multiple_of(o * 128, 128), 128)] for u, o in runs], axis=0)
        ACC[t, :, 512:768] += dot(res, onehot)

    @jax.named_call
    def pass_residual(e, c):
        for t in range(2):
            bytes_of(RG.at[e, t, pl.ds(*CHUNKS[c]), pl.ds(0, 2)], g_r.at[e, t, c, 0])
            if (e, c) in DIRECT_RESIDUALS:
                continue
            gather(e, t, c, 2).start()
            gather(e, t, c, 3).start()

    @jax.named_call
    def near_gradient(e, c):
        for t in range(2):
            accumulate(e, t, c, (0, 1, 3))

    @jax.named_call
    def gradient(e, c):
        for t in range(2):
            bytes_of(RG.at[e, t, pl.ds(*CHUNKS[c]), 0], g_r.at[e, t, c, 1])
            accumulate(e, t, c, (2,))

    @jax.named_call
    def core_sum(e):
        for t in range(2):
            for r in range(4):
                tile = 512 + (r // 2) * 128
                top, bottom = ACC[t, 0:32, tile:tile + 128], ACC[t, 32:64, tile:tile + 128]
                lanes = slice(r * 128, (r + 1) * 128)
                GS[e, 0, t, r] = ACC[t, 0:48, lanes]
                GS[e, 1, t, r, 0:16] = ACC[t, 48:64, lanes]
                if r % 2 == 0:
                    GS[e, 1, t, r, 16:48] = jnp.where(low, top, pltpu.roll(bottom, 64, 1))
                else:
                    GS[e, 1, t, r, 16:48] = jnp.where(low, pltpu.roll(top, 64, 1), bottom)
        gradients_across(e).start()
        gradients_across(e).wait_recv()
        for r in (2, 1, 3, 0):
            for t in range(2):
                GS[e, core, t, r] = GS[e, core, t, r] + GC[e, t, r]
                if r:
                    gradients(e, t, r).start()

    @jax.named_call
    def ring_sum(e):
        total = GS[e, core, 0, 0] + GS[e, core, 1, 0]
        for t in range(2):
            bytes_of(GR.at[e, t], q_r.at[e, t])
            for r in range(3):
                total = total + GR[e, t, r]
        DB[e, x, 0:48] = total
        DB[e, x, 48:56] = DIFF[...]
        for k in (2, 1, 3):
            chips(e, k).start()

    @jax.named_call
    def chip_sum(e):
        bytes_of(DB.at[e, pl.ds(0, 3)], d_r.at[e])
        return ((DB[e, 0] + DB[e, 1]) + DB[e, 2]) + DB[e, 3]

    def shared(e):
        totals_across(e).wait_recv()
        return kept(DC[e, 0, 0:48], DC[e, 1, 0:48])

    @jax.named_call
    def left(e):
        if e == 0:
            bytes_of(X, a_s.at[0])
        most = pl.ds(0, UNITS * 3 // 4)
        bytes_of(PL.at[e, :, most], rs_s.at[e])
        bytes_of(RG.at[e, :, most], g_s.at[e])
        bytes_of(CG.at[e], c_s.at[e])
        bytes_of(GR.at[e], q_s.at[e])
        bytes_of(DB.at[e, pl.ds(0, 3)], d_s.at[e])
        if e:
            weights_across(e).wait_send()
        gradients_across(e).wait_send()
        totals_across(e).wait_send()

    enter()
    prepare()
    met()
    send_weights(0)
    send_features(0)
    own(0).start()
    own(1).start()
    fetch(0).wait()
    fetch(1).wait()
    onehots()
    gather_weights(0)
    own(0).wait()
    own(1).wait()

    def arrived(c):
        wait_features(c)
        turn(c)
        logits(0, c)

    for s in range(NC + 5):
        for lag, stage in ((-1, send_features), (0, pass_features), (1, arrived), (2, add_passed), (3, softmax),
                           (4, pass_residual), (4, near_gradient), (5, gradient)):
            if 0 <= s - lag < NC:
                stage(*((s - lag,) if lag < 2 else (0, s - lag)))

    core_sum(0)
    ring_sum(0)
    grad = chip_sum(0)[0:48]
    step, pos = STEP[core], POS[core]
    half = MOM[core] + 0.5 * step * (grad - pos * IV[core])
    new = pos + step * half
    CS[1, core] = new.astype(BF16)
    send_weights(1)
    HALF[...] = half
    NEW[...] = new
    DC[0, core, 48:56] = jnp.zeros((8, 128), F32)
    DC[0, core, 0:48] = new
    totals_across(0).start()
    ACC[...] = jnp.zeros_like(ACC)

    coef_out[...], group = shared(0)
    group_out[...] = unpack(group)
    store(0).start()
    store(2).start()
    gather_weights(1)
    left(0)

    for stage in (logits, add_passed, softmax, pass_residual, near_gradient, gradient):
        for c in range(NC):
            stage(1, c)

    core_sum(1)
    ring_sum(1)
    total = chip_sum(1)

    @jax.named_call
    def finish():
        half, new, pos, old = HALF[...], NEW[...], POS[core], MOM[core]
        mom = half + 0.5 * STEP[core] * (total[0:48] - new * IV[core])
        state = 0.5 * ((new * new - pos * pos) * IV[core] + (mom * mom - old * old))
        EN[core * 16 + place[0] * 4 + place[1]] = total[48:56] + jnp.sum(state, axis=0, keepdims=True)
        for k in (15, 10, 11, 14, 5, 6, 7, 9, 13, 2, 8, 1, 3, 4, 12, 0):
            for other in range(2):
                if k or other:
                    energies(k, other).start()
        DC[1, core, 48:56] = jnp.zeros((8, 128), F32)
        DC[1, core, 0:48] = mom
        totals_across(1).start()
        coef_mom_out[...], group = shared(1)
        group_mom_out[...] = unpack(group)
        store(1).start()
        store(3).start()
    finish()
    left(1)
    for i in range(4):
        store(i).wait()

    @jax.named_call
    def total_energy():
        bytes_of(EN.at[pl.ds(0, 31)], e_r.at[0])
        terms = EN[0]
        for i in range(1, 32):
            terms = terms + EN[i]
        energy_ref[...] = jnp.broadcast_to(jnp.sum(terms, axis=1, keepdims=True), (8, 128))
        store(4).start()
        bytes_of(EN.at[pl.ds(0, 31)], e_s.at[0])
        store(4).wait()
    total_energy()


def hand_over(*refs):
    for source, target in zip(refs[:5], refs[5:]):
        target[...] = source[0:1, 0:1] if target.shape == (1, 1) else source[...]


def per_device(
    features, labels, groups, coefficients, coef_momentum, group_effects, group_momentum, log_scale
):
    rows = labels.shape[0]
    classes = coefficients.shape[1]
    rows_total = rows * lax.axis_size(DP)
    group_total = group_effects.shape[0] * lax.axis_size(FEAT)
    vmem = pl.BlockSpec(memory_space=pltpu.VMEM)
    dma = pltpu.SemaphoreType.DMA
    shapes = [(64, 128), (64, 128), (64, 64), (64, 64)]
    results = pl.pallas_call(
        lambda *refs: kernel(rows_total, group_total, *refs),
        out_shape=[jax.ShapeDtypeStruct(s, F32) for s in shapes + [(8, 128)]],
        in_specs=[pl.BlockSpec(memory_space=pl.ANY)] * 8,
        out_specs=[pl.BlockSpec(memory_space=pl.ANY)] * 5,
        scratch_shapes=[
            pltpu.VMEM((rows // 128, 128), jnp.int32), pltpu.VMEM((rows // 128, 128), jnp.int32),
            pltpu.VMEM((64, 128), F32), pltpu.VMEM((64, 128), F32),
            pltpu.VMEM((64, 64), F32), pltpu.VMEM((64, 64), F32), pltpu.VMEM((1, 64), F32),
            pltpu.VMEM((64, 128), F32), pltpu.VMEM((64, 128), F32),
            pltpu.VMEM((64, 64), F32), pltpu.VMEM((64, 64), F32), pltpu.VMEM((8, 128), F32),
            pltpu.VMEM((2, 4, BLOCK, 128), BF16),
            pltpu.VMEM((2, 2, BLOCK // 2, 128), BF16),
            pltpu.VMEM((2, UNITS, 768, UNIT), BF16),
            pltpu.VMEM((2, UNITS, UNIT, 256), BF16),
            pltpu.VMEM((2, 64, 768), BF16),
            pltpu.VMEM((2, 2, UNITS, 4, 64, 128), F32),
            pltpu.VMEM((2, 2, 2, UNITS, 32, 128), F32),
            pltpu.VMEM((2, 2, 2, UNITS, 64, 128), F32),
            pltpu.VMEM((2, 2, UNITS, 4, 64, 128), BF16),
            pltpu.VMEM((2, 2, 48, 128), BF16),
            pltpu.VMEM((2, 2, 3, 2, 48, 128), BF16),
            pltpu.VMEM((2, 64, 768), F32),
            pltpu.VMEM((2, 2, 2, 4, 48, 128), F32),
            pltpu.VMEM((2, 2, 4, 48, 128), F32),
            pltpu.VMEM((2, 2, 3, 48, 128), F32),
            pltpu.VMEM((2, 4, 56, 128), F32),
            pltpu.VMEM((2, 2, 56, 128), F32),
            pltpu.VMEM((32, 8, 128), F32),
            pltpu.VMEM((2, UNITS, 8, 128), F32),
            pltpu.VMEM((8, 128), F32),
            pltpu.VMEM((2, 48, 128), F32), pltpu.VMEM((2, 48, 128), F32), pltpu.VMEM((2, 48, 128), F32),
            pltpu.VMEM((2, 48, 128), F32), pltpu.VMEM((48, 128), F32), pltpu.VMEM((48, 128), F32),
            pltpu.VMEM((64, 128), F32),
            dma((2,)), dma((7,)), dma((5,)),
            dma((1,)), dma((2, NC, 2)),
            dma((2,)), dma((2, 2, NC, 2)),
            dma((2,)), dma((2, 2, NC, 2)),
            dma((2,)), dma((2, 2)),
            dma((2, 3)), dma((2, 3)),
            dma((2,)), dma((2, 2)),
            dma((2,)), dma((2,)),
            dma((1,)), dma((1,)),
        ],
        compiler_params=pltpu.CompilerParams(
            collective_id=0, has_side_effects=True, vmem_limit_bytes=58 * 2**20),
        name="leapfrog",
    )(features, labels.reshape(-1, 128), groups.reshape(-1, 128), coefficients.T, coef_momentum.T,
      group_effects, group_momentum, log_scale.reshape(1, -1))
    coef, coef_mom, group, group_mom, energy = pl.pallas_call(
        hand_over,
        out_shape=[jax.ShapeDtypeStruct(s, F32) for s in shapes + [(1, 1)]],
        in_specs=[vmem] * 5,
        out_specs=[vmem] * 5,
        name="hand_over",
    )(*results)
    return (coef.T, coef_mom.T, group, group_mom, energy[0, 0])


def solution(mesh):
    torus = Mesh(mesh.devices.reshape(4, 2, 4, 4), ("dp_0", "dp_1", "feat_0", "feat_1"))
    in_specs = (
        P(DP, FEAT),
        P(DP),
        P(DP),
        P(FEAT, None),
        P(FEAT, None),
        P(FEAT, None),
        P(FEAT, None),
        P(),
    )
    out_specs = (P(FEAT, None), P(FEAT, None), P(FEAT, None), P(FEAT, None), P())
    return jax.shard_map(
        per_device, mesh=torus, in_specs=in_specs, out_specs=out_specs, check_vma=False
    )
```
